256 devices in a mesh: pair: 64 (over x, z, y_hi), col: 2 (over y_lo), freq: 2 (over core).
Axes of the slice: x: 4, y: 4 (y_hi: 2, y_lo: 2; y = y_hi * 2 + y_lo), z: 8, core: 2. Of those that a mesh axis runs over, the one named last changes fastest.
Arguments:
- pair_matrix: bfloat16 [196608, 2048], P('pair', 'col'), may hold values from -0.0390625 to 0.0390625
- energies: float32 [196608], P('pair'), may hold values from 0.5 to 20
- omega: float32 [2], P('freq'), may hold values from 0.2 to 10
Outputs:
- chi: float32 [2048, 2, 2048], P('pair', 'freq', 'col')
The draws below stay inside these ranges and needn't reach their ends.
All inputs are finite; a program needn't handle non-finite values.
Results may differ from the reference program's by a relative error of at most 0.00053.
Values may be sent and summed in bfloat16 or wider, within the bound.
A program may use at most 128 MiB of HBM per device.

```python
import math
import jax
import jax.numpy as jnp
from jax import lax

K = 2048
NPAIR = 196608
NFREQ = 2


def strengthened(result, stream_key, source, target, shards_of, factor):
    def block_of(position):
        return (jnp.arange(result.shape[position]) // (result.shape[position] // shards_of)).reshape((-1,) + (1,) * (result.ndim - 1 - position))

    first = jax.random.permutation(stream_key, shards_of)[block_of(target)]
    far = (block_of(target) + shards_of // 2) % shards_of
    return jnp.where((block_of(source) == first) | (block_of(source) == far), factor * result, result)


def block_scale(rng, shape, pieces, low, top_value):
    loudness = 1.0
    for position, parts in pieces:
        steps = jax.random.uniform(jax.random.fold_in(jax.random.fold_in(rng, 6), position), (parts,), jnp.float32, low / len(pieces), top_value / len(pieces))
        loudness = loudness * jnp.repeat(jnp.exp(steps), shape[position] // parts).reshape((-1,) + (1,) * (len(shape) - 1 - position))
    return loudness


def noise_with(own_key, shape, deviation, bound, cuts, heavy, kind=jnp.bfloat16):
    result = deviation * jax.random.normal(own_key, shape, jnp.float32)
    if cuts:
        result = result * block_scale(own_key, shape, cuts, -0.22, 0.18)
    return jnp.clip(strengthened(result, jax.random.fold_in(own_key, 3), *heavy), -bound, bound).astype(kind)


def setup_inputs(seed: int = 0) -> dict:
    seeds = jax.random.split(jax.random.key(seed), 4)
    pair_matrix = noise_with(seeds[0], (NPAIR, K), NPAIR ** -0.5, 0.0390625, ((0, 64), (1, 2)), (0, 1, 64, 4.0))
    energies = jnp.clip(jnp.exp(math.log(20.0) - 3.6888795 * jax.random.uniform(seeds[1], (NPAIR,), jnp.float32) ** block_scale(seeds[1], (NPAIR,), ((0, 64),), -0.2, 0.2)), 0.5, 20.0)
    omega = jnp.clip(jnp.exp(math.log(10.0) - 3.912023 * jax.random.uniform(seeds[2], (NFREQ,), jnp.float32) ** block_scale(seeds[2], (NFREQ,), ((0, 2),), -0.2, 0.2)), 0.2, 10.0)
    return dict(pair_matrix=pair_matrix, energies=energies, omega=omega)


def reference(pair_matrix, energies, omega):
    width = math.gcd(NPAIR, 4096)
    count = NPAIR // width
    results = []
    for index in range(NFREQ):
        freq_value = omega[index]
        factor = jnp.sqrt(4.0 * energies / (energies * energies + freq_value * freq_value))

        def accumulate(total, block):
            begin = (block * width).astype(jnp.int32)
            rows = lax.dynamic_slice_in_dim(pair_matrix, begin, width, 0)
            scale = lax.dynamic_slice_in_dim(factor, begin, width, 0)
            rounded = (scale[:, None] * rows.astype(jnp.float32)).astype(jnp.bfloat16)
            rounded = lax.optimization_barrier(rounded).astype(jnp.float32)
            product = jnp.dot(rounded.T, rounded, precision=lax.Precision.HIGHEST)
            return (total - product, None)
        start = jnp.zeros((K, K), jnp.float32)
        total, unused = lax.scan(accumulate, start, jnp.arange(count, dtype=jnp.int32))
        results.append(total)
    return jnp.stack(results, axis=1)
```

```python
import jax
import jax.numpy as jnp
from jax import lax
from jax.experimental import pallas as pl
from jax.experimental.pallas import tpu as pltpu
from jax.sharding import Mesh
from jax.sharding import PartitionSpec as P

MESH = pl.DeviceIdType.MESH
ROWS = ("x", "z", "h")
ORDER = (0, 2, 1, 3)


def gram(left, right):
    return -lax.dot_general(
        left, right, (((0,), (0,)), ((), ())), preferred_element_type=jnp.float32
    )


def kernel(
    e_ref,
    w_ref,
    x_hbm,
    out_ref,
    own,
    fac,
    raw,
    other,
    part,
    relay,
    from_left,
    from_right,
    load_sem,
    y_send,
    y_recv,
    d_send,
    d_recv,
    x_send,
    relay_recv,
    left_recv,
    right_recv,
):
    x = lax.axis_index("x")
    low = lax.axis_index("l")
    core = lax.axis_index("f")
    right = lax.rem(x + 1, 4)
    left = lax.rem(x + 3, 4)
    pairs, cols = own.shape
    half = pairs // 2
    quarter = half // 2
    width = cols // 4
    mid = width // 2

    barrier = pltpu.get_barrier_semaphore()
    for peer in ({"x": right}, {"x": left}, {"l": 1 - low}, {"f": 1 - core}):
        pl.semaphore_signal(barrier, inc=1, device_id=peer, device_id_type=MESH)
    pl.semaphore_wait(barrier, 4)

    mine = pl.ds(pl.multiple_of(core * quarter, quarter), quarter)
    theirs = pl.ds(pl.multiple_of((1 - core) * quarter, quarter), quarter)
    leaving = pl.ds(pl.multiple_of((1 - low) * half + core * quarter, quarter), quarter)

    def y_copy(j):
        return pltpu.make_async_remote_copy(
            src_ref=x_hbm.at[leaving, pl.ds(j * width, width)],
            dst_ref=raw.at[j, mine],
            send_sem=y_send.at[j],
            recv_sem=y_recv.at[j],
            device_id={"l": 1 - low},
            device_id_type=MESH,
        )

    def d_copy(j, rows):
        return pltpu.make_async_remote_copy(
            src_ref=raw.at[j, rows],
            dst_ref=raw.at[j, rows],
            send_sem=d_send.at[j],
            recv_sem=d_recv.at[j],
            device_id={"f": 1 - core},
            device_id_type=MESH,
        )

    for j in ORDER:
        y_copy(j).start()
    loads = load_sem.shape[0]
    block = pairs // loads
    for b in range(loads):
        pltpu.make_async_copy(
            x_hbm.at[pl.ds(b * block, block)], own.at[pl.ds(b * block, block)], load_sem.at[b]
        ).start()

    freq = w_ref[0]

    @pl.loop(0, pairs // 128)
    def _(b):
        energy = e_ref[pl.ds(b, 1), :]
        value = jnp.sqrt(4.0 * energy / (energy * energy + freq * freq))
        fac[pl.ds(pl.multiple_of(b * 128, 128), 128), :] = jnp.broadcast_to(value, (128, 128)).T

    for b in range(loads):
        pltpu.make_async_copy(
            x_hbm.at[pl.ds(b * block, block)], own.at[pl.ds(b * block, block)], load_sem.at[b]
        ).wait()

        @pl.loop(0, block // 64)
        def _(i):
            rows = pl.ds(pl.multiple_of(b * block + i * 64, 64), 64)
            scale = fac[rows, :]
            for c in range(cols // 128):
                lanes = pl.ds(c * 128, 128)
                own[rows, lanes] = (scale * own[rows, lanes].astype(jnp.float32)).astype(jnp.bfloat16)

    def distance(k):
        dest = (2 * low if k < 4 else 2 * (1 - low)) + (k % 4) // 2
        return lax.rem(dest - x + 4, 4)

    def x_copy(k, side, to_right, relayed):
        rows = pl.ds(side * mid, mid)
        inbox = from_left if to_right else from_right
        inbox_sem = left_recv if to_right else right_recv
        return pltpu.make_async_remote_copy(
            src_ref=part.at[k, rows],
            dst_ref=relay.at[k] if relayed else inbox.at[k % 2, rows],
            send_sem=x_send.at[k, side],
            recv_sem=relay_recv.at[k] if relayed else inbox_sem.at[k % 2, side],
            device_id={"x": right if to_right else left},
            device_id_type=MESH,
        )

    def send_direct(k):
        far = distance(k)

        @pl.when(far == 2)
        def _():
            x_copy(k, 0, True, True).start()
            x_copy(k, 1, False, True).start()

        @pl.when(far == 1)
        def _():
            x_copy(k, 1, True, False).start()

        @pl.when(far == 3)
        def _():
            x_copy(k, 0, False, False).start()

    def send_relayed(k):
        far = distance(k)
        for away, side, to_right in ((1, 0, True), (3, 1, False)):

            @pl.when(far == away)
            def _():
                x_copy(k, side, to_right, True).wait_recv()

                @pl.loop(0, mid // 8)
                def _(i):
                    at = pl.multiple_of(i * 8, 8)
                    rows = pl.ds(side * mid + at, 8)
                    part[k, rows, :] = part[k, rows, :] + relay[k, pl.ds(at, 8), :]

                x_copy(k, side, to_right, False).start()

    def finish(k):
        @pl.when(distance(k) == 0)
        def _():
            for side in range(2):
                x_copy(k, side, True, False).wait_recv()
                x_copy(k, side, False, False).wait_recv()
            i = k % 2

            @pl.loop(0, width // 8)
            def _(r):
                at = pl.ds(pl.multiple_of(r * 8, 8), 8)
                out_ref[pl.ds(pl.multiple_of(i * width + r * 8, 8), 8), :] = (
                    part[k, at, :] + from_left[i, at, :] + from_right[i, at, :]
                )

        @pl.when(distance(k) != 0)
        def _():
            for side in range(2):
                x_copy(k, side, True, False).wait_send()

    for k in ORDER:
        part[k] = gram(own[:, k * width : (k + 1) * width], own[...])
        send_direct(k)

    pending = list(ORDER)
    mine_half = pl.ds(pl.multiple_of(low * half, half), half)
    for j in ORDER:
        y_copy(j).wait_recv()
        d_copy(j, mine).start()
        d_copy(j, theirs).wait_recv()

        @pl.loop(0, half // 64)
        def _(i):
            at = pl.multiple_of(i * 64, 64)
            scale = fac[pl.ds(pl.multiple_of(low * half + i * 64, 64), 64), :]
            for c in range(width // 128):
                lanes = pl.ds(c * 128, 128)
                other[pl.ds(at, 64), lanes] = (
                    scale * raw[j, pl.ds(at, 64), lanes].astype(jnp.float32)
                ).astype(jnp.bfloat16)

        part[4 + j] = gram(other[...], own[mine_half, :])
        send_direct(4 + j)
        send_relayed(pending.pop(0))
        pending.append(4 + j)
    for k in pending:
        send_relayed(k)
    for k in range(8):
        finish(k)
    for j in range(4):
        y_copy(j).wait_send()
        d_copy(j, mine).wait_send()


def column_sums(pair_matrix, energies, omega):
    pairs, cols = pair_matrix.shape
    width = cols // 4
    vmem, dma = pltpu.VMEM, pltpu.SemaphoreType.DMA
    loads = 6
    return pl.pallas_call(
        kernel,
        out_shape=jax.ShapeDtypeStruct((2 * width, cols), jnp.float32),
        in_specs=[
            pl.BlockSpec(memory_space=pltpu.VMEM),
            pl.BlockSpec(memory_space=pltpu.SMEM),
            pl.BlockSpec(memory_space=pl.ANY),
        ],
        out_specs=pl.BlockSpec(memory_space=pltpu.VMEM),
        scratch_shapes=[
            vmem((pairs, cols), jnp.bfloat16),
            vmem((pairs, 128), jnp.float32),
            vmem((4, pairs // 2, width), jnp.bfloat16),
            vmem((pairs // 2, width), jnp.bfloat16),
            vmem((8, width, cols), jnp.float32),
            vmem((8, width // 2, cols), jnp.float32),
            vmem((2, width, cols), jnp.float32),
            vmem((2, width, cols), jnp.float32),
            dma((loads,)),
            dma((4,)),
            dma((4,)),
            dma((4,)),
            dma((4,)),
            dma((8, 2)),
            dma((8,)),
            dma((2, 2)),
            dma((2, 2)),
        ],
        compiler_params=pltpu.CompilerParams(
            collective_id=0, has_side_effects=True, vmem_limit_bytes=60 * 1024 * 1024
        ),
    )(energies.reshape(pairs // 128, 128), omega, pair_matrix)


def per_device(pair_matrix, energies, omega):
    summed = column_sums(pair_matrix, energies, omega)
    summed = lax.psum_scatter(summed, "z", scatter_dimension=0, tiled=True)
    owned = lax.psum_scatter(summed, "h", scatter_dimension=0, tiled=True)
    rows, cols = owned.shape
    pieces = jnp.moveaxis(owned.reshape(rows, 2, 16, rows), 2, 0)
    pieces = lax.all_to_all(pieces, ("z", "h"), 0, 0, tiled=True)
    pieces = jnp.transpose(pieces, (2, 3, 0, 1)).reshape(2, rows, 16 * rows)
    x, low = lax.axis_index("x"), lax.axis_index("l")
    bit = lax.rem(x, 2)
    got = []
    for k in range(2):
        perm = [
            ((2 * (1 - m) + b) * 2 + m, (2 * m + (b ^ k)) * 2 + 1 - m) for m in range(2) for b in range(2)
        ]
        sent = jnp.where((bit + k) % 2 == 0, pieces[0], pieces[1])
        got.append(lax.ppermute(sent, ("x", "l"), perm))
    first = jnp.where(bit == 0, got[0], got[1])
    second = jnp.where(bit == 0, got[1], got[0])
    owned = owned + jnp.concatenate([first, second], axis=1)
    return owned[:, None, :]


def solution(mesh):
    finer = Mesh(mesh.devices.reshape(4, 8, 2, 2, 2), ("x", "z", "h", "l", "f"))
    return jax.shard_map(
        per_device,
        mesh=finer,
        in_specs=(P(ROWS, "l"), P(ROWS), P("f")),
        out_specs=P(ROWS, "f", "l"),
        check_vma=False,
    )
```

```python
import jax
import jax.numpy as jnp
from jax import lax
from jax.experimental import pallas as pl
from jax.experimental.pallas import tpu as pltpu
from jax.sharding import Mesh
from jax.sharding import PartitionSpec as P

MESH = pl.DeviceIdType.MESH
ROWS = ("x", "z", "h")


def gram(left, right):
    return -lax.dot_general(
        left, right, (((0,), (0,)), ((), ())), preferred_element_type=jnp.float32
    )


def aligned(value, size):
    return pl.ds(pl.multiple_of(value, size), size)


class Ring:
    def __init__(self, axis, n, block, inbox, send_sem, recv_sem):
        self.axis, self.n, self.block, self.inbox = axis, n, block, inbox
        self.send_sem, self.recv_sem = send_sem, recv_sem
        self.pos = lax.axis_index(axis)

    def first(self, way, side):
        return self.n // 2 if way == side else self.n // 2 - 1

    def toward(self, way, dist):
        return lax.rem(self.pos + (dist if way == 0 else self.n - dist), self.n)

    def copy(self, way, side, dist):
        return pltpu.make_async_remote_copy(
            src_ref=self.block(self.toward(way, dist), side),
            dst_ref=self.inbox.at[way, side, dist - 1],
            send_sem=self.send_sem.at[way, side, dist - 1],
            recv_sem=self.recv_sem.at[way, side, dist - 1],
            device_id={self.axis: self.toward(way, 1)},
            device_id_type=MESH,
        )

    def begin(self, way, side):
        self.copy(way, side, self.first(way, side)).start()

    def hop(self, way, side, dist):
        self.copy(way, side, dist + 1).wait_recv()
        held = self.block(self.toward(way, dist), side)
        came = self.inbox.at[way, side, dist]

        @pl.loop(0, held.shape[0] // 16)
        def _(i):
            rows = aligned(i * 16, 16)
            held[rows, :] = held[rows, :] + came[rows, :]

        self.copy(way, side, dist).start()

    def begin_all(self):
        for way, side in ((0, 0), (1, 1), (0, 1), (1, 0)):
            self.begin(way, side)

    def steps(self):
        out = []
        for dist in range(self.n // 2 - 1, 0, -1):
            out.append(((0, 0, dist), (1, 1, dist)))
            if dist > 1:
                out.append(((0, 1, dist - 1), (1, 0, dist - 1)))
        return out

    def arrived(self):
        for way in range(2):
            for side in range(2):
                self.copy(way, side, 1).wait_recv()

    def drain(self):
        for way in range(2):
            for side in range(2):
                for dist in range(self.first(way, side), 0, -1):
                    self.copy(way, side, dist).wait_send()


def kernel(
    e_ref,
    w_ref,
    x_hbm,
    out_ref,
    own,
    fac,
    raw,
    other,
    d_part,
    d_box,
    c_part,
    c_box,
    e_part,
    e_box,
    f_part,
    f_box,
    tile,
    tile_t,
    tile_box,
    d_tile,
    d_tile_box,
    in_d,
    in_n,
    in_t,
    load_sem,
    y_send,
    y_recv,
    s_send,
    s_recv,
    d_send,
    d_recv,
    c_send,
    c_recv,
    e_send,
    e_recv,
    f_send,
    f_recv,
    h_send,
    h_recv,
    in_d_sem,
    in_n_sem,
    in_t_sem,
    out_d_sem,
    out_n_sem,
    out_t_sem,
):
    x, z, h = lax.axis_index("x"), lax.axis_index("z"), lax.axis_index("h")
    low, core = lax.axis_index("l"), lax.axis_index("f")
    pairs, cols = own.shape
    half, width = pairs // 2, cols // 4
    quarter, mid = half // 2, width // 2
    div = lax.div

    barrier = pltpu.get_barrier_semaphore()
    peers = (
        {"x": lax.rem(x + 1, 4)},
        {"x": lax.rem(x + 3, 4)},
        {"z": lax.rem(z + 1, 8)},
        {"z": lax.rem(z + 7, 8)},
        {"h": 1 - h},
        {"l": 1 - low},
        {"f": 1 - core},
    )
    for peer in peers:
        pl.semaphore_signal(barrier, inc=1, device_id=peer, device_id_type=MESH)
    pl.semaphore_wait(barrier, len(peers))

    mine = aligned(core * quarter, quarter)
    theirs = aligned((1 - core) * quarter, quarter)
    leaving = aligned((1 - low) * half + core * quarter, quarter)

    def remote(src, dst, send, recv, peer):
        return pltpu.make_async_remote_copy(
            src_ref=src, dst_ref=dst, send_sem=send, recv_sem=recv, device_id=peer, device_id_type=MESH
        )

    def y_copy(j):
        src = x_hbm.at[leaving, pl.ds(j * width, width)]
        return remote(src, raw.at[j, mine], y_send.at[j], y_recv.at[j], {"l": 1 - low})

    def s_copy(j, rows):
        return remote(raw.at[j, rows], raw.at[j, rows], s_send.at[j], s_recv.at[j], {"f": 1 - core})

    for j in range(4):
        y_copy(j).start()
    loads = load_sem.shape[0]
    block = pairs // loads

    def load(b):
        rows = pl.ds(b * block, block)
        return pltpu.make_async_copy(x_hbm.at[rows], own.at[rows], load_sem.at[b])

    for b in range(loads):
        load(b).start()

    freq = w_ref[0]

    @pl.loop(0, pairs // 128)
    def _(b):
        energy = e_ref[pl.ds(b, 1), :]
        value = jnp.sqrt(4.0 * energy / (energy * energy + freq * freq))
        fac[aligned(b * 128, 128), :] = jnp.broadcast_to(value, (128, 128)).T

    for b in range(loads):
        load(b).wait()

        @pl.loop(0, block // 64)
        def _(i):
            rows = aligned(b * block + i * 64, 64)
            scale = fac[rows, :]
            for c in range(cols // 128):
                lanes = pl.ds(c * 128, 128)
                own[rows, lanes] = (scale * own[rows, lanes].astype(jnp.float32)).astype(jnp.bfloat16)

    ring_d = Ring("z", 8, lambda d, s: d_part.at[d, pl.ds(s * 64, 64)], d_box, d_send, d_recv)
    ring_f = Ring("x", 4, lambda d, s: f_part.at[d, pl.ds(s * 64, 64)], f_box, f_send, f_recv)
    ring_c = [
        Ring("x", 4, lambda d, s, j=j: c_part.at[j, d, pl.ds(s * mid, mid)], c_box.at[j], c_send.at[j], c_recv.at[j])
        for j in range(4)
    ]
    ring_e = [
        Ring("z", 8, lambda d, s, t=t: e_part.at[t, d, pl.ds(s * 64, 64)], e_box.at[t], e_send.at[t], e_recv.at[t])
        for t in range(2)
    ]

    def run(ring, step):
        for way, side, dist in ring.steps()[step]:
            ring.hop(way, side, dist)

    def own_pair(ways):
        first, second = (ring_d.toward(*way) for way in ways)
        lanes = [own[:, aligned(d * 128, 128)] for d in (first, second)]
        block = gram(jnp.concatenate(lanes, axis=1), own[...])
        d_part[first] = block[:128]
        d_part[second] = block[128:]

    mine_half = aligned(low * half, half)

    def cross(j):
        y_copy(j).wait_recv()
        s_copy(j, mine).start()
        s_copy(j, theirs).wait_recv()

        @pl.loop(0, half // 64)
        def _(i):
            rows = aligned(i * 64, 64)
            scale = fac[aligned(low * half + i * 64, 64), :]
            for c in range(width // 128):
                lanes = pl.ds(c * 128, 128)
                other[rows, lanes] = (scale * raw[j, rows, lanes].astype(jnp.float32)).astype(jnp.bfloat16)

        block = gram(other[...], own[mine_half, :])
        for d in range(4):
            c_part[j, d] = block[:, d * width : (d + 1) * width]
        ring_c[j].begin_all()

    def cross_x_done(j):
        ring_c[j].arrived()
        for side in range(2):
            for c in range(2):
                lanes = pl.ds(c * 128, 128)

                @pl.loop(0, mid // 16)
                def _(i):
                    rows = aligned(i * 16, 16)
                    e_part[j // 2, 2 * (2 * (j % 2) + side) + c, rows, :] = (
                        c_part[j, x, aligned(side * mid + i * 16, 16), lanes]
                        + c_box[j, 0, side, 0, rows, lanes]
                        + c_box[j, 1, side, 0, rows, lanes]
                    )

    def h_copy(t):
        return remote(tile.at[t], tile_box, h_send.at[0], h_recv.at[0], {"h": 1 - h})

    def n_copy(q):
        peer = {"x": 2 * (1 - low) + h, "z": 2 * div(z, 2) + q // 2, "h": jnp.int32(q % 2)}
        slot = 2 * x + lax.rem(z, 2)
        own_slot = (peer["x"] == x) & (peer["z"] == z) & (peer["h"] == h)
        return slot, own_slot, remote(
            tile.at[h, pl.ds(32 * q, 32)], in_n.at[slot], out_n_sem.at[q], in_n_sem.at[slot], peer
        )

    def t_copy(q):
        peer = {
            "x": 2 * low + div(x, 2),
            "z": 4 * lax.rem(x, 2) + 2 * lax.rem(z, 2) + q // 2,
            "h": jnp.int32(q % 2),
            "l": 1 - low,
        }
        slot = 4 * h + div(z, 2)
        return remote(
            tile_t.at[pl.ds(32 * q, 32)], in_t.at[slot], out_t_sem.at[q], in_t_sem.at[slot], peer
        )

    def cross_z_done(t):
        ring = ring_e[t]
        ring.arrived()
        for side in range(2):

            @pl.loop(0, 4)
            def _(i):
                rows = aligned(i * 16, 16)
                into = aligned(side * 64 + i * 16, 16)
                tile[t, into, :] = (
                    e_part[t, z, into, :] + e_box[t, 0, side, 0, rows, :] + e_box[t, 1, side, 0, rows, :]
                )

        @pl.when(h != t)
        def _():
            h_copy(t).start()

        @pl.when(h == t)
        def _():
            h_copy(t).wait_recv()
            total = tile[t] + tile_box[...]
            tile[t] = total
            tile_t[...] = total.T
            for q in range(4):
                t_copy(q).start()
                slot, own_slot, copy = n_copy(q)

                @pl.when(jnp.logical_not(own_slot))
                def _():
                    copy.start()

                @pl.when(own_slot)
                def _():
                    in_n[slot] = tile[t, pl.ds(32 * q, 32), :]

    def own_z_done():
        ring_d.arrived()
        for d in range(4):
            lanes = pl.ds(d * width, width)
            for side in range(2):

                @pl.loop(0, 4)
                def _(i):
                    rows = aligned(i * 16, 16)
                    into = aligned(side * 64 + i * 16, 16)
                    f_part[d, into, :] = (
                        d_part[z, into, lanes] + d_box[0, side, 0, rows, lanes] + d_box[1, side, 0, rows, lanes]
                    )
        ring_f.begin_all()

    def dh_copy():
        src = d_tile.at[aligned((1 - h) * 64, 64)]
        return remote(src, d_tile_box, h_send.at[1], h_recv.at[1], {"h": 1 - h})

    def own_x_done():
        ring_f.arrived()
        for side in range(2):

            @pl.loop(0, 4)
            def _(i):
                rows = aligned(i * 16, 16)
                into = aligned(side * 64 + i * 16, 16)
                d_tile[into, :] = f_part[x, into, :] + f_box[0, side, 0, rows, :] + f_box[1, side, 0, rows, :]

        dh_copy().start()

    def od_copy(q):
        peer = {"x": 2 * low + div(z, 4), "z": 2 * lax.rem(z, 4) + h, "h": jnp.int32(q)}
        own_slot = (peer["x"] == x) & (peer["z"] == z) & (peer["h"] == h)
        src = d_tile.at[aligned(h * 64 + 32 * q, 32)]
        return own_slot, remote(src, in_d.at[x], out_d_sem.at[q], in_d_sem.at[x], peer)

    def own_h_done():
        dh_copy().wait_recv()

        @pl.loop(0, 4)
        def _(i):
            into = aligned(h * 64 + i * 16, 16)
            d_tile[into, :] = d_tile[into, :] + d_tile_box[aligned(i * 16, 16), :]

        for q in range(2):
            own_slot, copy = od_copy(q)

            @pl.when(jnp.logical_not(own_slot))
            def _():
                copy.start()

            @pl.when(own_slot)
            def _():
                in_d[x] = d_tile[aligned(h * 64 + 32 * q, 32), :]

    own_pair(((0, 4), (0, 3)))
    ring_d.begin(0, 0)
    ring_d.begin(1, 1)
    ring_d.begin(0, 1)
    own_pair(((1, 3), (0, 2)))
    ring_d.begin(1, 0)
    own_pair(((1, 2), (0, 1)))
    own_pair(((1, 1), (0, 0)))
    cross(0)
    run(ring_d, 0)
    run(ring_c[0], 0)
    cross(1)
    run(ring_d, 1)
    run(ring_c[1], 0)
    cross_x_done(0)
    run(ring_d, 2)
    cross_x_done(1)
    ring_e[0].begin_all()
    cross(2)
    run(ring_d, 3)
    run(ring_c[2], 0)
    run(ring_e[0], 0)
    run(ring_e[0], 1)
    run(ring_e[0], 2)
    cross(3)
    run(ring_e[0], 3)
    run(ring_d, 4)
    run(ring_e[0], 4)
    cross_x_done(2)
    run(ring_c[3], 0)
    cross_z_done(0)
    cross_x_done(3)
    ring_e[1].begin_all()
    run(ring_e[1], 0)
    run(ring_e[1], 1)
    own_z_done()
    run(ring_e[1], 2)
    run(ring_e[1], 3)
    run(ring_f, 0)
    run(ring_e[1], 4)
    cross_z_done(1)
    own_x_done()
    own_h_done()

    @pl.when(div(x, 2) == low)
    def _():
        here = (4 * (x - 2 * low) + div(z, 2) == z) & (lax.rem(z, 2) == h)
        for s in range(4):

            @pl.when(jnp.logical_not(here & (x == s)))
            def _():
                remote(in_d.at[s], in_d.at[s], out_d_sem.at[0], in_d_sem.at[s], {"h": 1 - h}).wait_recv()

            out_ref[:, s * width : (s + 1) * width] = in_d[s]

    @pl.when(div(x, 2) != low)
    def _():
        here = x - 2 * (1 - low) == h
        for s in range(8):

            @pl.when(jnp.logical_not(here & (2 * x + lax.rem(z, 2) == s)))
            def _():
                remote(in_n.at[s], in_n.at[s], out_n_sem.at[0], in_n_sem.at[s], {"h": 1 - h}).wait_recv()

            remote(in_t.at[s], in_t.at[s], out_t_sem.at[0], in_t_sem.at[s], {"h": 1 - h}).wait_recv()
            out_ref[:, s * 128 : (s + 1) * 128] = in_n[s] + in_t[s]

    for j in range(4):
        y_copy(j).wait_send()
        s_copy(j, mine).wait_send()
    for ring in (ring_d, ring_f, *ring_c, *ring_e):
        ring.drain()
    h_copy(1 - h).wait_send()
    dh_copy().wait_send()
    for q in range(4):
        t_copy(q).wait_send()
        _, own_slot, n_out = n_copy(q)

        @pl.when(jnp.logical_not(own_slot))
        def _():
            n_out.wait_send()

    for q in range(2):
        own_slot, d_out = od_copy(q)

        @pl.when(jnp.logical_not(own_slot))
        def _():
            d_out.wait_send()


def per_device(pair_matrix, energies, omega):
    pairs, cols = pair_matrix.shape
    width = cols // 4
    dma = pltpu.SemaphoreType.DMA
    loads = 6

    def f32(*shape):
        return pltpu.VMEM(shape, jnp.float32)

    def bf16(*shape):
        return pltpu.VMEM(shape, jnp.bfloat16)

    owned = pl.pallas_call(
        kernel,
        out_shape=jax.ShapeDtypeStruct((32, cols), jnp.float32),
        in_specs=[
            pl.BlockSpec(memory_space=pltpu.VMEM),
            pl.BlockSpec(memory_space=pltpu.SMEM),
            pl.BlockSpec(memory_space=pl.ANY),
        ],
        out_specs=pl.BlockSpec(memory_space=pltpu.VMEM),
        scratch_shapes=[
            bf16(pairs, cols),
            f32(pairs, 128),
            bf16(4, pairs // 2, width),
            bf16(pairs // 2, width),
            f32(8, 128, cols),
            f32(2, 2, 4, 64, cols),
            f32(4, 4, width, width),
            f32(4, 2, 2, 2, width // 2, width),
            f32(2, 8, 128, 128),
            f32(2, 2, 2, 4, 64, 128),
            f32(4, 128, width),
            f32(2, 2, 2, 64, width),
            f32(2, 128, 128),
            f32(128, 128),
            f32(128, 128),
            f32(128, width),
            f32(64, width),
            f32(4, 32, width),
            f32(8, 32, 128),
            f32(8, 32, 128),
            dma((loads,)),
            dma((4,)),
            dma((4,)),
            dma((4,)),
            dma((4,)),
            dma((2, 2, 4)),
            dma((2, 2, 4)),
            dma((4, 2, 2, 2)),
            dma((4, 2, 2, 2)),
            dma((2, 2, 2, 4)),
            dma((2, 2, 2, 4)),
            dma((2, 2, 2)),
            dma((2, 2, 2)),
            dma((2,)),
            dma((2,)),
            dma((4,)),
            dma((8,)),
            dma((8,)),
            dma((2,)),
            dma((4,)),
            dma((4,)),
        ],
        compiler_params=pltpu.CompilerParams(
            collective_id=0, has_side_effects=True, vmem_limit_bytes=60 * 1024 * 1024
        ),
    )(energies.reshape(pairs // 128, 128), omega, pair_matrix)
    return owned[:, None, :]


def solution(mesh):
    finer = Mesh(mesh.devices.reshape(4, 8, 2, 2, 2), ("x", "z", "h", "l", "f"))
    return jax.shard_map(
        per_device,
        mesh=finer,
        in_specs=(P(ROWS, "l"), P(ROWS), P("f")),
        out_specs=P(ROWS, "f", "l"),
        check_vma=False,
    )
```

```python
import jax
import jax.numpy as jnp
from jax import lax
from jax.experimental import pallas as pl
from jax.experimental.pallas import tpu as pltpu
from jax.sharding import Mesh
from jax.sharding import PartitionSpec as P

MESH = pl.DeviceIdType.MESH
ROWS = ("x", "z", "h")
CHUNKS = ((0, 256), (256, 256), (512, 256), (768, 128), (896, 128))


def gram(left, right):
    return -lax.dot_general(
        left, right, (((0,), (0,)), ((), ())), preferred_element_type=jnp.float32
    )


def aligned(value, size, length=None):
    return pl.ds(pl.multiple_of(value, size), length or size)


class Ring:
    def __init__(self, axis, n, block, inbox, send_sem, recv_sem):
        self.axis, self.n, self.block, self.inbox = axis, n, block, inbox
        self.send_sem, self.recv_sem = send_sem, recv_sem
        self.pos = lax.axis_index(axis)

    def first(self, way, side):
        return self.n // 2 if way == side else self.n // 2 - 1

    def toward(self, way, dist):
        return lax.rem(self.pos + (dist if way == 0 else self.n - dist), self.n)

    def copy(self, way, side, dist):
        return pltpu.make_async_remote_copy(
            src_ref=self.block(self.toward(way, dist), side),
            dst_ref=self.inbox(way, side, dist - 1),
            send_sem=self.send_sem.at[way, side, dist - 1],
            recv_sem=self.recv_sem.at[way, side, dist - 1],
            device_id={self.axis: self.toward(way, 1)},
            device_id_type=MESH,
        )

    def begin(self, way, side):
        self.copy(way, side, self.first(way, side)).start()

    def hop(self, way, side, dist):
        self.copy(way, side, dist + 1).wait_recv()
        held = self.block(self.toward(way, dist), side)
        came = self.inbox(way, side, dist)

        @pl.loop(0, held.shape[0] // 16)
        def _(i):
            rows = aligned(i * 16, 16)
            held[rows, :] = held[rows, :] + came[rows, :]

        self.copy(way, side, dist).start()

    def begin_all(self):
        for way, side in ((0, 0), (1, 1), (0, 1), (1, 0)):
            self.begin(way, side)

    def steps(self):
        out = []
        for dist in range(self.n // 2 - 1, 0, -1):
            out.append(((0, 0, dist), (1, 1, dist)))
            if dist > 1:
                out.append(((0, 1, dist - 1), (1, 0, dist - 1)))
        return out

    def arrived(self):
        for way in range(2):
            for side in range(2):
                self.copy(way, side, 1).wait_recv()

    def drain(self):
        for way in range(2):
            for side in range(2):
                for dist in range(self.first(way, side), 0, -1):
                    self.copy(way, side, dist).wait_send()


def kernel(
    e_ref,
    w_ref,
    x_hbm,
    out_ref,
    own,
    fac,
    raw,
    other,
    d_part,
    d_box,
    c_part,
    c_box,
    e_part,
    e_box,
    f_part,
    f_box,
    tile,
    tile_t,
    tile_box,
    d_sum,
    d_sum_box,
    d_fin,
    pad,
    turned,
    in_d,
    in_dt,
    in_n,
    in_t,
    load_sem,
    y_send,
    y_recv,
    s_send,
    s_recv,
    d_send,
    d_recv,
    c_send,
    c_recv,
    e_send,
    e_recv,
    f_send,
    f_recv,
    h_send,
    h_recv,
    in_d_sem,
    in_dt_sem,
    in_n_sem,
    in_t_sem,
    out_d_sem,
    out_dt_sem,
    out_n_sem,
    out_t_sem,
):
    x, z, h = lax.axis_index("x"), lax.axis_index("z"), lax.axis_index("h")
    low, core = lax.axis_index("l"), lax.axis_index("f")
    pairs, cols = x_hbm.shape
    half, width = pairs // 2, cols // 4
    quarter = half // 2
    wide = d_part.shape[2]
    div = lax.div

    barrier = pltpu.get_barrier_semaphore()
    peers = (
        {"x": lax.rem(x + 1, 4)},
        {"x": lax.rem(x + 3, 4)},
        {"z": lax.rem(z + 1, 8)},
        {"z": lax.rem(z + 7, 8)},
        {"h": 1 - h},
        {"l": 1 - low},
        {"f": 1 - core},
    )
    for peer in peers:
        pl.semaphore_signal(barrier, inc=1, device_id=peer, device_id_type=MESH)
    pl.semaphore_wait(barrier, len(peers))

    mine = aligned(core * quarter, quarter)
    theirs = aligned((1 - core) * quarter, quarter)
    leaving = aligned((1 - low) * half + core * quarter, quarter)

    def remote(src, dst, send, recv, peer):
        return pltpu.make_async_remote_copy(
            src_ref=src, dst_ref=dst, send_sem=send, recv_sem=recv, device_id=peer, device_id_type=MESH
        )

    def y_copy(j):
        src = x_hbm.at[leaving, pl.ds(*CHUNKS[j])]
        return remote(src, raw[j].at[mine], y_send.at[j], y_recv.at[j], {"l": 1 - low})

    def s_copy(j, rows):
        return remote(raw[j].at[rows], raw[j].at[rows], s_send.at[j], s_recv.at[j], {"f": 1 - core})

    for j in range(len(CHUNKS)):
        y_copy(j).start()
    loads = load_sem.shape[0]
    block = pairs // loads

    def load(b):
        rows = pl.ds(b * block, block)
        return pltpu.make_async_copy(x_hbm.at[rows], own.at[rows, pl.ds(0, cols)], load_sem.at[b])

    for b in range(loads):
        load(b).start()

    freq = w_ref[0]

    @pl.loop(0, pairs // 128)
    def _(b):
        energy = e_ref[pl.ds(b, 1), :]
        value = jnp.sqrt(4.0 * energy / (energy * energy + freq * freq))
        fac[aligned(b * 128, 128), :] = jnp.broadcast_to(value, (128, 128)).T

    for b in range(loads):
        load(b).wait()

        @pl.loop(0, block // 64)
        def _(i):
            rows = aligned(b * block + i * 64, 64)
            scale = fac[rows, :]
            for c in range(cols // 128):
                lanes = pl.ds(c * 128, 128)
                scaled = (scale * own[rows, lanes].astype(jnp.float32)).astype(jnp.bfloat16)
                own[rows, lanes] = scaled
                if c < 5:
                    own[rows, pl.ds(cols + c * 128, 128)] = scaled

    ring_d = Ring(
        "z", 8, lambda d, s: d_part.at[d, pl.ds(s * 64, 64)], lambda *i: d_box.at[*i], d_send, d_recv
    )
    ring_f = Ring(
        "x", 4, lambda d, s: f_part.at[d, pl.ds(s * 16, 16)], lambda *i: f_box.at[*i], f_send, f_recv
    )

    def ring_of_chunk(j):
        first, size = CHUNKS[j]
        mid = size // 2

        def block(d, s):
            return c_part.at[d, pl.ds(first + s * mid, mid)]

        def inbox(way, side, k):
            return c_box.at[way, side, k, pl.ds(first // 2, mid)]

        return Ring("x", 4, block, inbox, c_send.at[j], c_recv.at[j])

    ring_c = [ring_of_chunk(j) for j in range(len(CHUNKS))]
    ring_e = [
        Ring(
            "z",
            8,
            lambda d, s, t=t: e_part.at[t, d, pl.ds(s * 64, 64)],
            lambda *i, t=t: e_box.at[t, *i],
            e_send.at[t],
            e_recv.at[t],
        )
        for t in range(2)
    ]

    def run(ring, step):
        for way, side, dist in ring.steps()[step]:
            ring.hop(way, side, dist)

    def own_pair(way, dist):
        one = ring_d.toward(way, dist)
        two = lax.rem(one + 1, 8)
        block = gram(own[:, aligned(one * 128, 128, 256)], own[:, aligned(one * 128, 128, wide + 128)])
        d_part[one] = block[:128, :wide]
        d_part[two] = block[128:, 128:]

    mine_half = aligned(low * half, half)

    def cross(j):
        first, size = CHUNKS[j]
        y_copy(j).wait_recv()
        s_copy(j, mine).start()
        s_copy(j, theirs).wait_recv()

        @pl.loop(0, half // 64)
        def _(i):
            rows = aligned(i * 64, 64)
            scale = fac[aligned(low * half + i * 64, 64), :]
            for c in range(size // 128):
                lanes = pl.ds(c * 128, 128)
                other[rows, lanes] = (scale * raw[j][rows, lanes].astype(jnp.float32)).astype(jnp.bfloat16)

        block = gram(other[:, :size], own[mine_half, :cols])
        for d in range(4):
            c_part[d, pl.ds(first, size), :] = block[:, d * width : (d + 1) * width]
        ring_c[j].begin_all()

    def cross_x_done(j):
        first, size = CHUNKS[j]
        mid = size // 2
        ring_c[j].arrived()
        for side in range(2):
            start = first + side * mid
            for c in range(2):
                lanes = pl.ds(c * 128, 128)

                @pl.loop(0, mid // 16)
                def _(i):
                    rows = aligned(first // 2 + i * 16, 16)
                    e_part[start // 512, 2 * (start % 512 // 128) + c, aligned(start % 128 + i * 16, 16), :] = (
                        c_part[x, aligned(start + i * 16, 16), lanes]
                        + c_box[0, side, 0, rows, lanes]
                        + c_box[1, side, 0, rows, lanes]
                    )

    def h_copy(t):
        return remote(tile.at[t], tile_box, h_send.at[0], h_recv.at[0], {"h": 1 - h})

    def n_copy(q):
        peer = {"x": 2 * (1 - low) + h, "z": 2 * div(z, 2) + q // 2, "h": jnp.int32(q % 2)}
        slot = 2 * x + lax.rem(z, 2)
        own_slot = (peer["x"] == x) & (peer["z"] == z) & (peer["h"] == h)
        return slot, own_slot, remote(
            tile.at[h, pl.ds(32 * q, 32)], in_n.at[slot], out_n_sem.at[q], in_n_sem.at[slot], peer
        )

    def t_copy(q):
        peer = {
            "x": 2 * low + div(x, 2),
            "z": 4 * lax.rem(x, 2) + 2 * lax.rem(z, 2) + q // 2,
            "h": jnp.int32(q % 2),
            "l": 1 - low,
        }
        slot = 4 * h + div(z, 2)
        return remote(
            tile_t.at[pl.ds(32 * q, 32)], in_t.at[slot], out_t_sem.at[q], in_t_sem.at[slot], peer
        )

    def cross_z_done(t):
        ring = ring_e[t]
        ring.arrived()
        for side in range(2):

            @pl.loop(0, 4)
            def _(i):
                rows = aligned(i * 16, 16)
                into = aligned(side * 64 + i * 16, 16)
                tile[t, into, :] = (
                    e_part[t, z, into, :] + e_box[t, 0, side, 0, rows, :] + e_box[t, 1, side, 0, rows, :]
                )

        @pl.when(h != t)
        def _():
            h_copy(t).start()

        @pl.when(h == t)
        def _():
            h_copy(t).wait_recv()
            total = tile[t] + tile_box[...]
            tile[t] = total
            tile_t[...] = total.T
            for q in range(4):
                t_copy(q).start()
                slot, own_slot, copy = n_copy(q)

                @pl.when(jnp.logical_not(own_slot))
                def _():
                    copy.start()

                @pl.when(own_slot)
                def _():
                    in_n[slot] = tile[t, pl.ds(32 * q, 32), :]

    def own_z_done():
        ring_d.arrived()
        for side in range(2):
            for part in range(2):
                d = 2 * side + part

                @pl.loop(0, 2)
                def _(i):
                    rows = aligned(part * 32 + i * 16, 16)
                    f_part[d, aligned(i * 16, 16), :] = (
                        d_part[z, aligned(d * 32 + i * 16, 16), :]
                        + d_box[0, side, 0, rows, :]
                        + d_box[1, side, 0, rows, :]
                    )

        ring_f.begin_all()

    def dh_copy():
        return remote(d_sum, d_sum_box, h_send.at[1], h_recv.at[1], {"h": 1 - h})

    def own_x_done():
        ring_f.arrived()
        for side in range(2):
            rows = pl.ds(side * 16, 16)
            d_sum[rows, :] = f_part[x, rows, :] + f_box[0, side, 0] + f_box[1, side, 0]
        dh_copy().start()

    def straight_copy():
        peer = {"x": 2 * low + div(z, 4), "z": 2 * lax.rem(z, 4) + div(x, 2)}
        stays = (peer["x"] == x) & (peer["z"] == z)
        return stays, remote(d_fin, in_d, out_d_sem.at[0], in_d_sem.at[0], peer)

    def turned_copy(t, k):
        j = lax.rem(z + t, 8)
        peer = {"x": 2 * low + div(j, 4), "z": 2 * lax.rem(j, 4) + k}
        stays = (peer["x"] == x) & (peer["z"] == z)
        src = turned.at[t - 1, aligned(64 * k + 32 * h, 32)]
        return stays, src, remote(src, in_dt.at[t - 1, x], out_dt_sem.at[t - 1, k], in_dt_sem.at[t - 1, x], peer)

    def own_h_done():
        dh_copy().wait_recv()
        d_fin[...] = d_sum[...] + d_sum_box[...]

        @pl.when(h == lax.rem(x, 2))
        def _():
            stays, copy = straight_copy()

            @pl.when(jnp.logical_not(stays))
            def _():
                copy.start()

            @pl.when(stays)
            def _():
                in_d[...] = d_fin[...]

        pad[...] = jnp.zeros_like(pad)
        for t in range(1, 4):
            pad[aligned(x * 32, 32), :] = d_fin[:, t * 128 : (t + 1) * 128]
            turned[t - 1] = pad[...].T
            for k in range(2):
                stays, src, copy = turned_copy(t, k)

                @pl.when(jnp.logical_not(stays))
                def _():
                    copy.start()

                @pl.when(stays)
                def _():
                    in_dt[t - 1, x] = src[...]

    own_pair(0, 3)
    ring_d.begin(0, 0)
    ring_d.begin(1, 1)
    ring_d.begin(0, 1)
    own_pair(1, 3)
    ring_d.begin(1, 0)
    own_pair(0, 1)
    own_pair(1, 1)
    cross(0)
    run(ring_d, 0)
    run(ring_d, 1)
    run(ring_c[0], 0)
    cross(1)
    run(ring_d, 2)
    run(ring_d, 3)
    cross_x_done(0)
    run(ring_c[1], 0)
    run(ring_d, 4)
    cross(2)
    cross_x_done(1)
    ring_e[0].begin_all()
    cross(3)
    run(ring_c[2], 0)
    run(ring_e[0], 0)
    own_z_done()
    cross(4)
    run(ring_c[3], 0)
    run(ring_e[0], 1)
    run(ring_f, 0)
    cross_x_done(2)
    run(ring_e[0], 2)
    run(ring_c[4], 0)
    cross_x_done(3)
    run(ring_e[0], 3)
    own_x_done()
    cross_x_done(4)
    ring_e[1].begin_all()
    run(ring_e[0], 4)
    own_h_done()
    run(ring_e[1], 0)
    cross_z_done(0)
    for step in range(1, 5):
        run(ring_e[1], step)
    cross_z_done(1)

    @pl.when(div(x, 2) == low)
    def _():
        j = 4 * (x - 2 * low) + div(z, 2)
        p = 2 * lax.rem(z, 2) + h

        @pl.when(jnp.logical_not((z == j) & (x == p)))
        def _():
            remote(in_d, in_d, out_d_sem.at[0], in_d_sem.at[0], {"h": 1 - h}).wait_recv()

        for t in range(5):
            out_ref[:, aligned(lax.rem(j + t, 8) * 128, 128)] = in_d[:, t * 128 : (t + 1) * 128]
        for t in range(1, 4):
            source = lax.rem(j + 8 - t, 8)
            for q in range(4):

                @pl.when(jnp.logical_not((z == source) & (x == q)))
                def _():
                    box = in_dt.at[t - 1, q]
                    remote(box, box, out_dt_sem.at[0, 0], in_dt_sem.at[t - 1, q], {"h": 1 - h}).wait_recv()

            out_ref[:, aligned(source * 128, 128)] = (
                in_dt[t - 1, 0] + in_dt[t - 1, 1] + in_dt[t - 1, 2] + in_dt[t - 1, 3]
            )

    @pl.when(div(x, 2) != low)
    def _():
        here = x - 2 * (1 - low) == h
        for s in range(8):

            @pl.when(jnp.logical_not(here & (2 * x + lax.rem(z, 2) == s)))
            def _():
                remote(in_n.at[s], in_n.at[s], out_n_sem.at[0], in_n_sem.at[s], {"h": 1 - h}).wait_recv()

            remote(in_t.at[s], in_t.at[s], out_t_sem.at[0], in_t_sem.at[s], {"h": 1 - h}).wait_recv()
            out_ref[:, s * 128 : (s + 1) * 128] = in_n[s] + in_t[s]

    for j in range(len(CHUNKS)):
        y_copy(j).wait_send()
        s_copy(j, mine).wait_send()
    for ring in (ring_d, ring_f, *ring_c, *ring_e):
        ring.drain()
    h_copy(1 - h).wait_send()
    dh_copy().wait_send()
    for q in range(4):
        t_copy(q).wait_send()
        _, own_slot, n_out = n_copy(q)

        @pl.when(jnp.logical_not(own_slot))
        def _():
            n_out.wait_send()

    stays, straight = straight_copy()

    @pl.when((h == lax.rem(x, 2)) & jnp.logical_not(stays))
    def _():
        straight.wait_send()

    for t in range(1, 4):
        for k in range(2):
            kept, _, turn = turned_copy(t, k)

            @pl.when(jnp.logical_not(kept))
            def _():
                turn.wait_send()


def per_device(pair_matrix, energies, omega):
    pairs, cols = pair_matrix.shape
    width = cols // 4
    dma = pltpu.SemaphoreType.DMA
    loads, chunks = 6, len(CHUNKS)

    def f32(*shape):
        return pltpu.VMEM(shape, jnp.float32)

    def bf16(*shape):
        return pltpu.VMEM(shape, jnp.bfloat16)

    owned = pl.pallas_call(
        kernel,
        out_shape=jax.ShapeDtypeStruct((32, cols), jnp.float32),
        in_specs=[
            pl.BlockSpec(memory_space=pltpu.VMEM),
            pl.BlockSpec(memory_space=pltpu.SMEM),
            pl.BlockSpec(memory_space=pl.ANY),
        ],
        out_specs=pl.BlockSpec(memory_space=pltpu.VMEM),
        scratch_shapes=[
            bf16(pairs, 13 * 128),
            f32(pairs, 128),
            [bf16(pairs // 2, size) for _, size in CHUNKS],
            bf16(pairs // 2, width),
            f32(8, 128, 640),
            f32(2, 2, 4, 64, 640),
            f32(4, cols, width),
            f32(2, 2, 2, cols // 2, width),
            f32(2, 8, 128, 128),
            f32(2, 2, 2, 4, 64, 128),
            f32(4, 32, 640),
            f32(2, 2, 2, 16, 640),
            f32(2, 128, 128),
            f32(128, 128),
            f32(128, 128),
            f32(32, 640),
            f32(32, 640),
            f32(32, 640),
            f32(128, 128),
            f32(3, 128, 128),
            f32(32, 640),
            f32(3, 4, 32, 128),
            f32(8, 32, 128),
            f32(8, 32, 128),
            dma((loads,)),
            dma((chunks,)),
            dma((chunks,)),
            dma((chunks,)),
            dma((chunks,)),
            dma((2, 2, 4)),
            dma((2, 2, 4)),
            dma((chunks, 2, 2, 2)),
            dma((chunks, 2, 2, 2)),
            dma((2, 2, 2, 4)),
            dma((2, 2, 2, 4)),
            dma((2, 2, 2)),
            dma((2, 2, 2)),
            dma((2,)),
            dma((2,)),
            dma((1,)),
            dma((3, 4)),
            dma((8,)),
            dma((8,)),
            dma((1,)),
            dma((3, 2)),
            dma((4,)),
            dma((4,)),
        ],
        compiler_params=pltpu.CompilerParams(
            collective_id=0, has_side_effects=True, vmem_limit_bytes=60 * 1024 * 1024
        ),
    )(energies.reshape(pairs // 128, 128), omega, pair_matrix)
    return owned[:, None, :]


def solution(mesh):
    finer = Mesh(mesh.devices.reshape(4, 8, 2, 2, 2), ("x", "z", "h", "l", "f"))
    return jax.shard_map(
        per_device,
        mesh=finer,
        in_specs=(P(ROWS, "l"), P(ROWS), P("f")),
        out_specs=P(ROWS, "f", "l"),
        check_vma=False,
    )
```

```python
import jax
import jax.numpy as jnp
from jax import lax
from jax.experimental import pallas as pl
from jax.experimental.pallas import tpu as pltpu
from jax.sharding import Mesh
from jax.sharding import PartitionSpec as P

MESH = pl.DeviceIdType.MESH
ROWS = ("x", "z", "h")
CHUNKS = ((0, 256), (256, 256), (512, 256), (768, 128), (896, 128))


def gram(left, right):
    return -lax.dot_general(
        left, right, (((0,), (0,)), ((), ())), preferred_element_type=jnp.float32
    )


def aligned(value, size, length=None):
    return pl.ds(pl.multiple_of(value, size), length or size)


class Ring:
    def __init__(self, axis, n, block, inbox, send_sem, recv_sem):
        self.axis, self.n, self.block, self.inbox = axis, n, block, inbox
        self.send_sem, self.recv_sem = send_sem, recv_sem
        self.pos = lax.axis_index(axis)

    def first(self, way, side):
        return self.n // 2 if way == side else self.n // 2 - 1

    def toward(self, way, dist):
        return lax.rem(self.pos + (dist if way == 0 else self.n - dist), self.n)

    def copy(self, way, side, dist):
        return pltpu.make_async_remote_copy(
            src_ref=self.block(self.toward(way, dist), side),
            dst_ref=self.inbox(way, side, dist - 1),
            send_sem=self.send_sem.at[way, side, dist - 1],
            recv_sem=self.recv_sem.at[way, side, dist - 1],
            device_id={self.axis: self.toward(way, 1)},
            device_id_type=MESH,
        )

    def begin(self, way, side):
        self.copy(way, side, self.first(way, side)).start()

    def hop(self, way, side, dist):
        self.copy(way, side, dist + 1).wait_recv()
        held = self.block(self.toward(way, dist), side)
        came = self.inbox(way, side, dist)

        @pl.loop(0, held.shape[0] // 16)
        def _(i):
            rows = aligned(i * 16, 16)
            held[rows, :] = held[rows, :] + came[rows, :]

        self.copy(way, side, dist).start()

    def begin_all(self):
        for way, side in ((0, 0), (1, 1), (0, 1), (1, 0)):
            self.begin(way, side)

    def steps(self):
        out = []
        for dist in range(self.n // 2 - 1, 0, -1):
            out.append(((0, 0, dist), (1, 1, dist)))
            if dist > 1:
                out.append(((0, 1, dist - 1), (1, 0, dist - 1)))
        return out

    def arrived(self):
        for way in range(2):
            for side in range(2):
                self.copy(way, side, 1).wait_recv()

    def drain(self):
        for way in range(2):
            for side in range(2):
                for dist in range(self.first(way, side), 0, -1):
                    self.copy(way, side, dist).wait_send()


class CodedRing(Ring):
    def __init__(self, *ring, staged, scale):
        super().__init__(*ring)
        self.staged, (self.enc, self.dec) = staged, scale

    def copy(self, way, side, dist):
        return pltpu.make_async_remote_copy(
            src_ref=self.staged(way, side, dist - 1),
            dst_ref=self.inbox(way, side, dist - 1),
            send_sem=self.send_sem.at[way, side, dist - 1],
            recv_sem=self.recv_sem.at[way, side, dist - 1],
            device_id={self.axis: self.toward(way, 1)},
            device_id_type=MESH,
        )

    def encode(self, value):
        scaled = value * self.enc[:1, : value.shape[1]]
        power = scaled * scaled
        power = power * power
        power = power * power
        return jnp.where(scaled < 0, -power, power).astype(jnp.bfloat16)

    def decode(self, code):
        power = code.astype(jnp.float32)
        fourth = lax.rsqrt(lax.rsqrt(jnp.maximum(jnp.abs(power), 1e-37)))
        root = fourth * lax.rsqrt(fourth) * self.dec[:1, : code.shape[1]]
        return jnp.where(power < 0, -root, root)

    def stage(self, way, side, dist, came=None):
        held = self.block(self.toward(way, dist), side)
        staged = self.staged(way, side, dist - 1)

        @pl.loop(0, held.shape[0] // 64)
        def _(i):
            rows = aligned(i * 64, 64)
            value = held[rows, :]
            if came is not None:
                value = value + self.decode(came[rows, :])
            staged[rows, :] = self.encode(value)

        self.copy(way, side, dist).start()

    def begin(self, way, side):
        self.stage(way, side, self.first(way, side))

    def hop(self, way, side, dist):
        self.copy(way, side, dist + 1).wait_recv()
        self.stage(way, side, dist, self.inbox(way, side, dist))


def kernel(
    e_ref,
    w_ref,
    x_hbm,
    out_ref,
    own,
    fac,
    raw,
    other,
    d_part,
    d_box,
    c_part,
    c_box,
    c_code,
    b_own,
    b_low,
    b_both,
    b_far,
    enc,
    dec,
    e_part,
    e_box,
    f_part,
    f_box,
    tile,
    tile_t,
    tile_box,
    d_sum,
    d_sum_box,
    d_fin,
    pad,
    turned,
    in_d,
    in_dt,
    in_n,
    in_t,
    load_sem,
    y_send,
    y_recv,
    s_send,
    s_recv,
    d_send,
    d_recv,
    c_send,
    c_recv,
    b_send,
    b_recv,
    e_send,
    e_recv,
    f_send,
    f_recv,
    h_send,
    h_recv,
    in_d_sem,
    in_dt_sem,
    in_n_sem,
    in_t_sem,
    out_d_sem,
    out_dt_sem,
    out_n_sem,
    out_t_sem,
):
    x, z, h = lax.axis_index("x"), lax.axis_index("z"), lax.axis_index("h")
    low, core = lax.axis_index("l"), lax.axis_index("f")
    pairs, cols = x_hbm.shape
    half, width = pairs // 2, cols // 4
    quarter = half // 2
    wide = d_part.shape[2]
    div = lax.div

    barrier = pltpu.get_barrier_semaphore()
    peers = (
        {"x": lax.rem(x + 1, 4)},
        {"x": lax.rem(x + 2, 4)},
        {"x": lax.rem(x + 3, 4)},
        {"x": lax.rem(x + 3, 4), "l": 1 - low},
        {"z": lax.rem(z + 1, 8)},
        {"z": lax.rem(z + 7, 8)},
        {"h": 1 - h},
        {"l": 1 - low},
        {"f": 1 - core},
    )
    for peer in peers:
        pl.semaphore_signal(barrier, inc=1, device_id=peer, device_id_type=MESH)
    pl.semaphore_wait(barrier, len(peers))

    mine = aligned(core * quarter, quarter)
    theirs = aligned((1 - core) * quarter, quarter)
    leaving = aligned((1 - low) * half + core * quarter, quarter)

    def remote(src, dst, send, recv, peer):
        return pltpu.make_async_remote_copy(
            src_ref=src, dst_ref=dst, send_sem=send, recv_sem=recv, device_id=peer, device_id_type=MESH
        )

    def y_copy(j):
        src = x_hbm.at[leaving, pl.ds(*CHUNKS[j])]
        return remote(src, raw[j].at[mine], y_send.at[j], y_recv.at[j], {"l": 1 - low})

    def s_copy(j, rows):
        return remote(raw[j].at[rows], raw[j].at[rows], s_send.at[j], s_recv.at[j], {"f": 1 - core})

    for j in range(len(CHUNKS)):
        y_copy(j).start()
    loads = load_sem.shape[0]
    block = pairs // loads

    def load(b):
        rows = pl.ds(b * block, block)
        return pltpu.make_async_copy(x_hbm.at[rows], own.at[rows, pl.ds(0, cols)], load_sem.at[b])

    for b in range(loads):
        load(b).start()

    freq = w_ref[0]

    @pl.loop(0, pairs // 128)
    def _(b):
        energy = e_ref[pl.ds(b, 1), :]
        value = jnp.sqrt(4.0 * energy / (energy * energy + freq * freq))
        fac[aligned(b * 128, 128), :] = jnp.broadcast_to(value, (128, 128)).T

    for b in range(loads):
        load(b).wait()

        @pl.loop(0, block // 64)
        def _(i):
            rows = aligned(b * block + i * 64, 64)
            scale = fac[rows, :]
            for c in range(cols // 128):
                lanes = pl.ds(c * 128, 128)
                scaled = (scale * own[rows, lanes].astype(jnp.float32)).astype(jnp.bfloat16)
                own[rows, lanes] = scaled
                if c < 5:
                    own[rows, pl.ds(cols + c * 128, 128)] = scaled

    ring_d = Ring(
        "z", 8, lambda d, s: d_part.at[d, pl.ds(s * 64, 64)], lambda *i: d_box.at[*i], d_send, d_recv
    )
    ring_f = Ring(
        "x", 4, lambda d, s: f_part.at[d, pl.ds(s * 16, 16)], lambda *i: f_box.at[*i], f_send, f_recv
    )

    def ring_of_chunk(j):
        first, size = CHUNKS[j]
        mid = size // 2

        def block(d, s):
            return c_part.at[d, pl.ds(first + s * mid, mid)]

        def inbox(way, side, k):
            return c_box.at[way, side, k, pl.ds(first // 2, mid)]

        def staged(way, side, k):
            return c_code.at[way, side, k, pl.ds(first // 2, mid)]

        return CodedRing(
            "x", 4, block, inbox, c_send.at[j], c_recv.at[j], staged=staged, scale=(enc, dec)
        )

    ring_c = [ring_of_chunk(j) for j in range(len(CHUNKS))]
    ring_e = [
        Ring(
            "z",
            8,
            lambda d, s, t=t: e_part.at[t, d, pl.ds(s * 64, 64)],
            lambda *i, t=t: e_box.at[t, *i],
            e_send.at[t],
            e_recv.at[t],
        )
        for t in range(2)
    ]

    def run(ring, step):
        for way, side, dist in ring.steps()[step]:
            ring.hop(way, side, dist)

    def own_pair(way, dist):
        one = ring_d.toward(way, dist)
        two = lax.rem(one + 1, 8)
        block = gram(own[:, aligned(one * 128, 128, 256)], own[:, aligned(one * 128, 128, wide + 128)])
        d_part[one] = block[:128, :wide]
        d_part[two] = block[128:, 128:]

    mine_half = aligned(low * half, half)

    def cross(j):
        first, size = CHUNKS[j]
        y_copy(j).wait_recv()
        s_copy(j, mine).start()
        s_copy(j, theirs).wait_recv()

        @pl.loop(0, half // 64)
        def _(i):
            rows = aligned(i * 64, 64)
            scale = fac[aligned(low * half + i * 64, 64), :]
            for c in range(size // 128):
                lanes = pl.ds(c * 128, 128)
                other[rows, lanes] = (scale * raw[j][rows, lanes].astype(jnp.float32)).astype(jnp.bfloat16)

        block = gram(other[:, :size], own[mine_half, :cols])
        for d in range(4):
            c_part[d, pl.ds(first, size), :] = block[:, d * width : (d + 1) * width]

    def b_copy(k):
        if k == 0:
            return remote(b_own, b_low, b_send.at[0], b_recv.at[0], {"x": lax.rem(x + 1, 4), "l": 1 - low})
        return remote(b_both, b_far.at[k - 1], b_send.at[k], b_recv.at[k], {"x": lax.rem(x + k, 4)})

    def bound_own():
        most = jnp.abs(d_part[0, :, :128])
        for d in range(1, 8):
            most = jnp.maximum(most, jnp.abs(d_part[d, :, :128]))
        b_own[...] = jnp.full(b_own.shape, jnp.max(most), jnp.float32)
        b_copy(0).start()

    def bound_both():
        b_copy(0).wait_recv()
        b_both[...] = jnp.maximum(b_own[...], b_low[...])
        for k in range(1, 4):
            b_copy(k).start()

    def bound_all():
        most = b_both[...]
        for k in range(1, 4):
            b_copy(k).wait_recv()
            most = jnp.maximum(most, b_far[k - 1])
        most = jnp.broadcast_to(4.0 * jnp.maximum(most[:1, :], 1e-30), (8, 128))
        for c in range(2):
            enc[:, c * 128 : (c + 1) * 128] = 32768.0 / most
            dec[:, c * 128 : (c + 1) * 128] = most / 32768.0

    def cross_x_done(j):
        first, size = CHUNKS[j]
        mid = size // 2
        ring_c[j].arrived()
        for side in range(2):
            start = first + side * mid
            for c in range(2):
                lanes = pl.ds(c * 128, 128)

                @pl.loop(0, mid // 64)
                def _(i):
                    rows = aligned(first // 2 + i * 64, 64)
                    e_part[start // 512, 2 * (start % 512 // 128) + c, aligned(start % 128 + i * 64, 64), :] = (
                        c_part[x, aligned(start + i * 64, 64), lanes]
                        + ring_c[j].decode(c_box[0, side, 0, rows, lanes])
                        + ring_c[j].decode(c_box[1, side, 0, rows, lanes])
                    )

    def h_copy(t):
        return remote(tile.at[t], tile_box, h_send.at[0], h_recv.at[0], {"h": 1 - h})

    def n_copy(q):
        peer = {"x": 2 * (1 - low) + h, "z": 2 * div(z, 2) + q // 2, "h": jnp.int32(q % 2)}
        slot = 2 * x + lax.rem(z, 2)
        own_slot = (peer["x"] == x) & (peer["z"] == z) & (peer["h"] == h)
        return slot, own_slot, remote(
            tile.at[h, pl.ds(32 * q, 32)], in_n.at[slot], out_n_sem.at[q], in_n_sem.at[slot], peer
        )

    def t_copy(q):
        peer = {
            "x": 2 * low + div(x, 2),
            "z": 4 * lax.rem(x, 2) + 2 * lax.rem(z, 2) + q // 2,
            "h": jnp.int32(q % 2),
            "l": 1 - low,
        }
        slot = 4 * h + div(z, 2)
        return remote(
            tile_t.at[pl.ds(32 * q, 32)], in_t.at[slot], out_t_sem.at[q], in_t_sem.at[slot], peer
        )

    def cross_z_done(t):
        ring = ring_e[t]
        ring.arrived()
        for side in range(2):

            @pl.loop(0, 4)
            def _(i):
                rows = aligned(i * 16, 16)
                into = aligned(side * 64 + i * 16, 16)
                tile[t, into, :] = (
                    e_part[t, z, into, :] + e_box[t, 0, side, 0, rows, :] + e_box[t, 1, side, 0, rows, :]
                )

        @pl.when(h != t)
        def _():
            h_copy(t).start()

        @pl.when(h == t)
        def _():
            h_copy(t).wait_recv()
            total = tile[t] + tile_box[...]
            tile[t] = total
            tile_t[...] = total.T
            for q in range(4):
                t_copy(q).start()
                slot, own_slot, copy = n_copy(q)

                @pl.when(jnp.logical_not(own_slot))
                def _():
                    copy.start()

                @pl.when(own_slot)
                def _():
                    in_n[slot] = tile[t, pl.ds(32 * q, 32), :]

    def own_z_done():
        ring_d.arrived()
        for side in range(2):
            for part in range(2):
                d = 2 * side + part

                @pl.loop(0, 2)
                def _(i):
                    rows = aligned(part * 32 + i * 16, 16)
                    f_part[d, aligned(i * 16, 16), :] = (
                        d_part[z, aligned(d * 32 + i * 16, 16), :]
                        + d_box[0, side, 0, rows, :]
                        + d_box[1, side, 0, rows, :]
                    )

        ring_f.begin_all()

    def dh_copy():
        return remote(d_sum, d_sum_box, h_send.at[1], h_recv.at[1], {"h": 1 - h})

    def own_x_done():
        ring_f.arrived()
        for side in range(2):
            rows = pl.ds(side * 16, 16)
            d_sum[rows, :] = f_part[x, rows, :] + f_box[0, side, 0] + f_box[1, side, 0]
        dh_copy().start()

    def straight_copy():
        peer = {"x": 2 * low + div(z, 4), "z": 2 * lax.rem(z, 4) + div(x, 2)}
        stays = (peer["x"] == x) & (peer["z"] == z)
        return stays, remote(d_fin, in_d, out_d_sem.at[0], in_d_sem.at[0], peer)

    def turned_copy(t, k):
        j = lax.rem(z + t, 8)
        peer = {"x": 2 * low + div(j, 4), "z": 2 * lax.rem(j, 4) + k}
        stays = (peer["x"] == x) & (peer["z"] == z)
        src = turned.at[t - 1, aligned(64 * k + 32 * h, 32)]
        return stays, src, remote(src, in_dt.at[t - 1, x], out_dt_sem.at[t - 1, k], in_dt_sem.at[t - 1, x], peer)

    def own_h_done():
        dh_copy().wait_recv()
        d_fin[...] = d_sum[...] + d_sum_box[...]

        @pl.when(h == lax.rem(x, 2))
        def _():
            stays, copy = straight_copy()

            @pl.when(jnp.logical_not(stays))
            def _():
                copy.start()

            @pl.when(stays)
            def _():
                in_d[...] = d_fin[...]

        pad[...] = jnp.zeros_like(pad)
        for t in range(1, 4):
            pad[aligned(x * 32, 32), :] = d_fin[:, t * 128 : (t + 1) * 128]
            turned[t - 1] = pad[...].T
            for k in range(2):
                stays, src, copy = turned_copy(t, k)

                @pl.when(jnp.logical_not(stays))
                def _():
                    copy.start()

                @pl.when(stays)
                def _():
                    in_dt[t - 1, x] = src[...]

    own_pair(0, 3)
    ring_d.begin(0, 0)
    ring_d.begin(1, 1)
    ring_d.begin(0, 1)
    own_pair(1, 3)
    ring_d.begin(1, 0)
    own_pair(0, 1)
    own_pair(1, 1)
    bound_own()
    cross(0)
    bound_both()
    run(ring_d, 0)
    bound_all()
    ring_c[0].begin_all()
    run(ring_d, 1)
    run(ring_c[0], 0)
    cross(1)
    ring_c[1].begin_all()
    run(ring_d, 2)
    cross_x_done(0)
    run(ring_d, 3)
    run(ring_c[1], 0)
    run(ring_d, 4)
    cross(2)
    ring_c[2].begin_all()
    cross_x_done(1)
    ring_e[0].begin_all()
    own_z_done()
    cross(3)
    ring_c[3].begin_all()
    run(ring_c[2], 0)
    run(ring_e[0], 0)
    run(ring_f, 0)
    cross(4)
    ring_c[4].begin_all()
    run(ring_c[3], 0)
    cross_x_done(2)
    run(ring_e[0], 1)
    run(ring_c[4], 0)
    own_x_done()
    cross_x_done(3)
    cross_x_done(4)
    ring_e[1].begin_all()
    run(ring_e[0], 2)
    run(ring_e[1], 0)
    own_h_done()
    run(ring_e[0], 3)
    run(ring_e[1], 1)
    run(ring_e[0], 4)
    run(ring_e[1], 2)
    cross_z_done(0)
    run(ring_e[1], 3)
    run(ring_e[1], 4)
    cross_z_done(1)

    @pl.when(div(x, 2) == low)
    def _():
        j = 4 * (x - 2 * low) + div(z, 2)
        p = 2 * lax.rem(z, 2) + h

        @pl.when(jnp.logical_not((z == j) & (x == p)))
        def _():
            remote(in_d, in_d, out_d_sem.at[0], in_d_sem.at[0], {"h": 1 - h}).wait_recv()

        for t in range(5):
            out_ref[:, aligned(lax.rem(j + t, 8) * 128, 128)] = in_d[:, t * 128 : (t + 1) * 128]
        for t in range(1, 4):
            source = lax.rem(j + 8 - t, 8)
            for q in range(4):

                @pl.when(jnp.logical_not((z == source) & (x == q)))
                def _():
                    box = in_dt.at[t - 1, q]
                    remote(box, box, out_dt_sem.at[0, 0], in_dt_sem.at[t - 1, q], {"h": 1 - h}).wait_recv()

            out_ref[:, aligned(source * 128, 128)] = (
                in_dt[t - 1, 0] + in_dt[t - 1, 1] + in_dt[t - 1, 2] + in_dt[t - 1, 3]
            )

    @pl.when(div(x, 2) != low)
    def _():
        here = x - 2 * (1 - low) == h
        for s in range(8):

            @pl.when(jnp.logical_not(here & (2 * x + lax.rem(z, 2) == s)))
            def _():
                remote(in_n.at[s], in_n.at[s], out_n_sem.at[0], in_n_sem.at[s], {"h": 1 - h}).wait_recv()

            remote(in_t.at[s], in_t.at[s], out_t_sem.at[0], in_t_sem.at[s], {"h": 1 - h}).wait_recv()
            out_ref[:, s * 128 : (s + 1) * 128] = in_n[s] + in_t[s]

    for j in range(len(CHUNKS)):
        y_copy(j).wait_send()
        s_copy(j, mine).wait_send()
    for ring in (ring_d, ring_f, *ring_c, *ring_e):
        ring.drain()
    h_copy(1 - h).wait_send()
    for k in range(4):
        b_copy(k).wait_send()
    dh_copy().wait_send()
    for q in range(4):
        t_copy(q).wait_send()
        _, own_slot, n_out = n_copy(q)

        @pl.when(jnp.logical_not(own_slot))
        def _():
            n_out.wait_send()

    stays, straight = straight_copy()

    @pl.when((h == lax.rem(x, 2)) & jnp.logical_not(stays))
    def _():
        straight.wait_send()

    for t in range(1, 4):
        for k in range(2):
            kept, _, turn = turned_copy(t, k)

            @pl.when(jnp.logical_not(kept))
            def _():
                turn.wait_send()


def per_device(pair_matrix, energies, omega):
    pairs, cols = pair_matrix.shape
    width = cols // 4
    dma = pltpu.SemaphoreType.DMA
    loads, chunks = 6, len(CHUNKS)

    def f32(*shape):
        return pltpu.VMEM(shape, jnp.float32)

    def bf16(*shape):
        return pltpu.VMEM(shape, jnp.bfloat16)

    owned = pl.pallas_call(
        kernel,
        out_shape=jax.ShapeDtypeStruct((32, cols), jnp.float32),
        in_specs=[
            pl.BlockSpec(memory_space=pltpu.VMEM),
            pl.BlockSpec(memory_space=pltpu.SMEM),
            pl.BlockSpec(memory_space=pl.ANY),
        ],
        out_specs=pl.BlockSpec(memory_space=pltpu.VMEM),
        scratch_shapes=[
            bf16(pairs, 13 * 128),
            f32(pairs, 128),
            [bf16(pairs // 2, size) for _, size in CHUNKS],
            bf16(pairs // 2, width),
            f32(8, 128, 640),
            f32(2, 2, 4, 64, 640),
            f32(4, cols, width),
            bf16(2, 2, 2, cols // 2, width),
            bf16(2, 2, 2, cols // 2, width),
            f32(8, 128),
            f32(8, 128),
            f32(8, 128),
            f32(3, 8, 128),
            f32(8, width),
            f32(8, width),
            f32(2, 8, 128, 128),
            f32(2, 2, 2, 4, 64, 128),
            f32(4, 32, 640),
            f32(2, 2, 2, 16, 640),
            f32(2, 128, 128),
            f32(128, 128),
            f32(128, 128),
            f32(32, 640),
            f32(32, 640),
            f32(32, 640),
            f32(128, 128),
            f32(3, 128, 128),
            f32(32, 640),
            f32(3, 4, 32, 128),
            f32(8, 32, 128),
            f32(8, 32, 128),
            dma((loads,)),
            dma((chunks,)),
            dma((chunks,)),
            dma((chunks,)),
            dma((chunks,)),
            dma((2, 2, 4)),
            dma((2, 2, 4)),
            dma((chunks, 2, 2, 2)),
            dma((chunks, 2, 2, 2)),
            dma((4,)),
            dma((4,)),
            dma((2, 2, 2, 4)),
            dma((2, 2, 2, 4)),
            dma((2, 2, 2)),
            dma((2, 2, 2)),
            dma((2,)),
            dma((2,)),
            dma((1,)),
            dma((3, 4)),
            dma((8,)),
            dma((8,)),
            dma((1,)),
            dma((3, 2)),
            dma((4,)),
            dma((4,)),
        ],
        compiler_params=pltpu.CompilerParams(
            collective_id=0, has_side_effects=True, vmem_limit_bytes=60 * 1024 * 1024
        ),
    )(energies.reshape(pairs // 128, 128), omega, pair_matrix)
    return owned[:, None, :]


def solution(mesh):
    finer = Mesh(mesh.devices.reshape(4, 8, 2, 2, 2), ("x", "z", "h", "l", "f"))
    return jax.shard_map(
        per_device,
        mesh=finer,
        in_specs=(P(ROWS, "l"), P(ROWS), P("f")),
        out_specs=P(ROWS, "f", "l"),
        check_vma=False,
    )
```

```python
import jax
import jax.numpy as jnp
from jax import lax
from jax.experimental import pallas as pl
from jax.experimental.pallas import tpu as pltpu
from jax.sharding import Mesh
from jax.sharding import PartitionSpec as P

MESH = pl.DeviceIdType.MESH
ROWS = ("x", "z", "h")
CHUNKS = ((0, 256), (256, 256), (512, 256), (768, 128), (896, 128))


def gram(left, right):
    return -lax.dot_general(
        left, right, (((0,), (0,)), ((), ())), preferred_element_type=jnp.float32
    )


def aligned(value, size, length=None):
    return pl.ds(pl.multiple_of(value, size), length or size)


class Ring:
    def __init__(self, axis, n, block, inbox, send_sem, recv_sem):
        self.axis, self.n, self.block, self.inbox = axis, n, block, inbox
        self.send_sem, self.recv_sem = send_sem, recv_sem
        self.pos = lax.axis_index(axis)

    def first(self, way, side):
        return self.n // 2 if way == side else self.n // 2 - 1

    def toward(self, way, dist):
        return lax.rem(self.pos + (dist if way == 0 else self.n - dist), self.n)

    def copy(self, way, side, dist):
        return pltpu.make_async_remote_copy(
            src_ref=self.block(self.toward(way, dist), side),
            dst_ref=self.inbox(way, side, dist - 1),
            send_sem=self.send_sem.at[way, side, dist - 1],
            recv_sem=self.recv_sem.at[way, side, dist - 1],
            device_id={self.axis: self.toward(way, 1)},
            device_id_type=MESH,
        )

    def begin(self, way, side):
        self.copy(way, side, self.first(way, side)).start()

    def hop(self, way, side, dist):
        self.copy(way, side, dist + 1).wait_recv()
        held = self.block(self.toward(way, dist), side)
        came = self.inbox(way, side, dist)

        @pl.loop(0, held.shape[0] // 16)
        def _(i):
            rows = aligned(i * 16, 16)
            held[rows, :] = held[rows, :] + came[rows, :]

        self.copy(way, side, dist).start()

    def begin_all(self):
        for way, side in ((0, 0), (1, 1), (0, 1), (1, 0)):
            self.begin(way, side)

    def steps(self):
        out = []
        for dist in range(self.n // 2 - 1, 0, -1):
            out.append(((0, 0, dist), (1, 1, dist)))
            if dist > 1:
                out.append(((0, 1, dist - 1), (1, 0, dist - 1)))
        return out

    def arrived(self):
        for way in range(2):
            for side in range(2):
                self.copy(way, side, 1).wait_recv()

    def drain(self):
        for way in range(2):
            for side in range(2):
                for dist in range(self.first(way, side), 0, -1):
                    self.copy(way, side, dist).wait_send()


class CodedRing(Ring):
    def __init__(self, *ring, staged, scale):
        super().__init__(*ring)
        self.staged, (self.enc, self.dec) = staged, scale

    def copy(self, way, side, dist):
        return pltpu.make_async_remote_copy(
            src_ref=self.staged(way, side, dist - 1),
            dst_ref=self.inbox(way, side, dist - 1),
            send_sem=self.send_sem.at[way, side, dist - 1],
            recv_sem=self.recv_sem.at[way, side, dist - 1],
            device_id={self.axis: self.toward(way, 1)},
            device_id_type=MESH,
        )

    def encode(self, value):
        scaled = value * self.enc[:1, : value.shape[1]]
        power = scaled * scaled
        power = power * power
        power = power * power
        return jnp.where(scaled < 0, -power, power).astype(jnp.bfloat16)

    def decode(self, code):
        power = code.astype(jnp.float32)
        fourth = lax.rsqrt(lax.rsqrt(jnp.maximum(jnp.abs(power), 1e-37)))
        root = fourth * lax.rsqrt(fourth) * self.dec[:1, : code.shape[1]]
        return jnp.where(power < 0, -root, root)

    def stage(self, way, side, dist, came=None):
        held = self.block(self.toward(way, dist), side)
        staged = self.staged(way, side, dist - 1)

        @pl.loop(0, held.shape[0] // 64)
        def _(i):
            rows = aligned(i * 64, 64)
            value = held[rows, :]
            if came is not None:
                value = value + self.decode(came[rows, :])
            staged[rows, :] = self.encode(value)

        self.copy(way, side, dist).start()

    def begin(self, way, side):
        self.stage(way, side, self.first(way, side))

    def hop(self, way, side, dist):
        self.copy(way, side, dist + 1).wait_recv()
        self.stage(way, side, dist, self.inbox(way, side, dist))


def kernel(
    e_ref,
    w_ref,
    x_hbm,
    out_ref,
    own,
    fac,
    raw,
    other,
    d_part,
    d_box,
    c_part,
    c_box,
    c_code,
    b_own,
    b_low,
    b_both,
    b_far,
    enc,
    dec,
    e_part,
    e_box,
    f_part,
    f_box,
    tile,
    tile_t,
    d_sum,
    d_sum_box,
    d_fin,
    pad,
    turned,
    in_d,
    in_dt,
    in_n,
    in_t,
    load_sem,
    y_send,
    y_recv,
    s_send,
    s_recv,
    d_send,
    d_recv,
    c_send,
    c_recv,
    b_send,
    b_recv,
    e_send,
    e_recv,
    f_send,
    f_recv,
    h_send,
    h_recv,
    in_d_sem,
    in_dt_sem,
    in_n_sem,
    in_t_sem,
    out_d_sem,
    out_dt_sem,
    out_n_sem,
    out_t_sem,
):
    x, z, h = lax.axis_index("x"), lax.axis_index("z"), lax.axis_index("h")
    low, core = lax.axis_index("l"), lax.axis_index("f")
    pairs, cols = x_hbm.shape
    half, width = pairs // 2, cols // 4
    quarter = half // 2
    wide = d_part.shape[2]
    div = lax.div

    barrier = pltpu.get_barrier_semaphore()
    peers = (
        {"x": lax.rem(x + 1, 4)},
        {"x": lax.rem(x + 2, 4)},
        {"x": lax.rem(x + 3, 4)},
        {"x": lax.rem(x + 3, 4), "l": 1 - low},
        {"z": lax.rem(z + 1, 8)},
        {"z": lax.rem(z + 7, 8)},
        {"h": 1 - h},
        {"l": 1 - low},
        {"f": 1 - core},
    )
    for peer in peers:
        pl.semaphore_signal(barrier, inc=1, device_id=peer, device_id_type=MESH)
    pl.semaphore_wait(barrier, len(peers))

    mine = aligned(core * quarter, quarter)
    theirs = aligned((1 - core) * quarter, quarter)
    leaving = aligned((1 - low) * half + core * quarter, quarter)

    def remote(src, dst, send, recv, peer):
        return pltpu.make_async_remote_copy(
            src_ref=src, dst_ref=dst, send_sem=send, recv_sem=recv, device_id=peer, device_id_type=MESH
        )

    def y_copy(j):
        src = x_hbm.at[leaving, pl.ds(*CHUNKS[j])]
        return remote(src, raw[j].at[mine], y_send.at[j], y_recv.at[j], {"l": 1 - low})

    def s_copy(j, rows):
        return remote(raw[j].at[rows], raw[j].at[rows], s_send.at[j], s_recv.at[j], {"f": 1 - core})

    for j in range(len(CHUNKS)):
        y_copy(j).start()
    loads = load_sem.shape[0]
    block = pairs // loads

    def load(b):
        rows = pl.ds(b * block, block)
        return pltpu.make_async_copy(x_hbm.at[rows], own.at[rows, pl.ds(0, cols)], load_sem.at[b])

    for b in range(loads):
        load(b).start()

    freq = w_ref[0]

    @pl.loop(0, pairs // 128)
    def _(b):
        energy = e_ref[pl.ds(b, 1), :]
        value = jnp.sqrt(4.0 * energy / (energy * energy + freq * freq))
        fac[aligned(b * 128, 128), :] = jnp.broadcast_to(value, (128, 128)).T

    for b in range(loads):
        load(b).wait()

        @pl.loop(0, block // 64)
        def _(i):
            rows = aligned(b * block + i * 64, 64)
            scale = fac[rows, :]
            for c in range(cols // 128):
                lanes = pl.ds(c * 128, 128)
                scaled = (scale * own[rows, lanes].astype(jnp.float32)).astype(jnp.bfloat16)
                own[rows, lanes] = scaled
                if c < 5:
                    own[rows, pl.ds(cols + c * 128, 128)] = scaled

    ring_d = Ring(
        "z", 8, lambda d, s: d_part.at[d, pl.ds(s * 64, 64)], lambda *i: d_box.at[*i], d_send, d_recv
    )
    ring_f = Ring(
        "x", 4, lambda d, s: f_part.at[d, pl.ds(s * 16, 16)], lambda *i: f_box.at[*i], f_send, f_recv
    )

    def ring_of_chunk(j):
        first, size = CHUNKS[j]
        mid = size // 2

        def block(d, s):
            return c_part.at[d, pl.ds(first + s * mid, mid)]

        def inbox(way, side, k):
            return c_box.at[way, side, k, pl.ds(first // 2, mid)]

        def staged(way, side, k):
            return c_code.at[way, side, k, pl.ds(first // 2, mid)]

        return CodedRing(
            "x", 4, block, inbox, c_send.at[j], c_recv.at[j], staged=staged, scale=(enc, dec)
        )

    ring_c = [ring_of_chunk(j) for j in range(len(CHUNKS))]
    ring_e = [
        Ring(
            "z",
            8,
            lambda d, s, t=t: e_part.at[t, d, pl.ds(s * 64, 64)],
            lambda *i, t=t: e_box.at[t, *i],
            e_send.at[t],
            e_recv.at[t],
        )
        for t in range(2)
    ]

    def run(ring, step):
        for way, side, dist in ring.steps()[step]:
            ring.hop(way, side, dist)

    def own_pair(way, dist):
        one = ring_d.toward(way, dist)
        two = lax.rem(one + 1, 8)
        block = gram(own[:, aligned(one * 128, 128, 256)], own[:, aligned(one * 128, 128, wide + 128)])
        d_part[one] = block[:128, :wide]
        d_part[two] = block[128:, 128:]

    mine_half = aligned(low * half, half)

    def cross(j):
        first, size = CHUNKS[j]
        y_copy(j).wait_recv()
        s_copy(j, mine).start()
        s_copy(j, theirs).wait_recv()

        @pl.loop(0, half // 64)
        def _(i):
            rows = aligned(i * 64, 64)
            scale = fac[aligned(low * half + i * 64, 64), :]
            for c in range(size // 128):
                lanes = pl.ds(c * 128, 128)
                other[rows, lanes] = (scale * raw[j][rows, lanes].astype(jnp.float32)).astype(jnp.bfloat16)

        block = gram(other[:, :size], own[mine_half, :cols])
        for d in range(4):
            c_part[d, pl.ds(first, size), :] = block[:, d * width : (d + 1) * width]

    def b_copy(k):
        if k == 0:
            return remote(b_own, b_low, b_send.at[0], b_recv.at[0], {"x": lax.rem(x + 1, 4), "l": 1 - low})
        return remote(b_both, b_far.at[k - 1], b_send.at[k], b_recv.at[k], {"x": lax.rem(x + k, 4)})

    def bound_own():
        most = jnp.abs(d_part[0, :, :128])
        for d in range(1, 8):
            most = jnp.maximum(most, jnp.abs(d_part[d, :, :128]))
        b_own[...] = jnp.full(b_own.shape, jnp.max(most), jnp.float32)
        b_copy(0).start()

    def bound_both():
        b_copy(0).wait_recv()
        b_both[...] = jnp.maximum(b_own[...], b_low[...])
        for k in range(1, 4):
            b_copy(k).start()

    def bound_all():
        most = b_both[...]
        for k in range(1, 4):
            b_copy(k).wait_recv()
            most = jnp.maximum(most, b_far[k - 1])
        most = jnp.broadcast_to(4.0 * jnp.maximum(most[:1, :], 1e-30), (8, 128))
        for c in range(2):
            enc[:, c * 128 : (c + 1) * 128] = 32768.0 / most
            dec[:, c * 128 : (c + 1) * 128] = most / 32768.0

    def cross_x_done(j):
        first, size = CHUNKS[j]
        mid = size // 2
        ring_c[j].arrived()
        for side in range(2):
            start = first + side * mid
            for c in range(2):
                lanes = pl.ds(c * 128, 128)

                @pl.loop(0, mid // 64)
                def _(i):
                    rows = aligned(first // 2 + i * 64, 64)
                    e_part[start // 512, 2 * (start % 512 // 128) + c, aligned(start % 128 + i * 64, 64), :] = (
                        c_part[x, aligned(start + i * 64, 64), lanes]
                        + ring_c[j].decode(c_box[0, side, 0, rows, lanes])
                        + ring_c[j].decode(c_box[1, side, 0, rows, lanes])
                    )

    def n_copy(t, q):
        peer = {"x": 2 * (1 - low) + t, "z": 2 * div(z, 2) + q // 2, "h": jnp.int32(q % 2)}
        slot = 2 * x + lax.rem(z, 2)
        own_slot = (peer["x"] == x) & (peer["z"] == z) & (peer["h"] == h)
        return slot, own_slot, remote(
            tile.at[t, pl.ds(32 * q, 32)], in_n.at[h, slot], out_n_sem.at[t, q], in_n_sem.at[h, slot], peer
        )

    def t_copy(t, q):
        peer = {
            "x": 2 * low + div(x, 2),
            "z": 4 * lax.rem(x, 2) + 2 * lax.rem(z, 2) + q // 2,
            "h": jnp.int32(q % 2),
            "l": 1 - low,
        }
        slot = 4 * t + div(z, 2)
        return remote(
            tile_t.at[t, pl.ds(32 * q, 32)], in_t.at[h, slot], out_t_sem.at[t, q], in_t_sem.at[h, slot], peer
        )

    def cross_z_done(t):
        ring = ring_e[t]
        ring.arrived()
        for side in range(2):

            @pl.loop(0, 4)
            def _(i):
                rows = aligned(i * 16, 16)
                into = aligned(side * 64 + i * 16, 16)
                tile[t, into, :] = (
                    e_part[t, z, into, :] + e_box[t, 0, side, 0, rows, :] + e_box[t, 1, side, 0, rows, :]
                )

        tile_t[t] = tile[t].T
        for q in range(4):
            t_copy(t, q).start()
            slot, own_slot, copy = n_copy(t, q)

            @pl.when(jnp.logical_not(own_slot))
            def _():
                copy.start()

            @pl.when(own_slot)
            def _():
                in_n[h, slot] = tile[t, pl.ds(32 * q, 32), :]

    def own_z_done():
        ring_d.arrived()
        for side in range(2):
            for part in range(2):
                d = 2 * side + part

                @pl.loop(0, 2)
                def _(i):
                    rows = aligned(part * 32 + i * 16, 16)
                    f_part[d, aligned(i * 16, 16), :] = (
                        d_part[z, aligned(d * 32 + i * 16, 16), :]
                        + d_box[0, side, 0, rows, :]
                        + d_box[1, side, 0, rows, :]
                    )

        ring_f.begin_all()

    def dh_copy():
        return remote(d_sum, d_sum_box, h_send.at[1], h_recv.at[1], {"h": 1 - h})

    def own_x_done():
        ring_f.arrived()
        for side in range(2):
            rows = pl.ds(side * 16, 16)
            d_sum[rows, :] = f_part[x, rows, :] + f_box[0, side, 0] + f_box[1, side, 0]
        dh_copy().start()

    def straight_copy():
        peer = {"x": 2 * low + div(z, 4), "z": 2 * lax.rem(z, 4) + div(x, 2)}
        stays = (peer["x"] == x) & (peer["z"] == z)
        return stays, remote(d_fin, in_d, out_d_sem.at[0], in_d_sem.at[0], peer)

    def turned_copy(t, k):
        j = lax.rem(z + t, 8)
        peer = {"x": 2 * low + div(j, 4), "z": 2 * lax.rem(j, 4) + k}
        stays = (peer["x"] == x) & (peer["z"] == z)
        src = turned.at[t - 1, aligned(64 * k + 32 * h, 32)]
        return stays, src, remote(src, in_dt.at[t - 1, x], out_dt_sem.at[t - 1, k], in_dt_sem.at[t - 1, x], peer)

    def own_h_done():
        dh_copy().wait_recv()
        d_fin[...] = d_sum[...] + d_sum_box[...]

        @pl.when(h == lax.rem(x, 2))
        def _():
            stays, copy = straight_copy()

            @pl.when(jnp.logical_not(stays))
            def _():
                copy.start()

            @pl.when(stays)
            def _():
                in_d[...] = d_fin[...]

        pad[...] = jnp.zeros_like(pad)
        for t in range(1, 4):
            pad[aligned(x * 32, 32), :] = d_fin[:, t * 128 : (t + 1) * 128]
            turned[t - 1] = pad[...].T
            for k in range(2):
                stays, src, copy = turned_copy(t, k)

                @pl.when(jnp.logical_not(stays))
                def _():
                    copy.start()

                @pl.when(stays)
                def _():
                    in_dt[t - 1, x] = src[...]

    own_pair(0, 3)
    ring_d.begin(0, 0)
    ring_d.begin(1, 1)
    ring_d.begin(0, 1)
    own_pair(1, 3)
    ring_d.begin(1, 0)
    own_pair(0, 1)
    own_pair(1, 1)
    bound_own()
    cross(0)
    bound_both()
    run(ring_d, 0)
    bound_all()
    ring_c[0].begin_all()
    run(ring_d, 1)
    run(ring_c[0], 0)
    cross(1)
    ring_c[1].begin_all()
    run(ring_d, 2)
    cross_x_done(0)
    run(ring_d, 3)
    run(ring_c[1], 0)
    run(ring_d, 4)
    cross(2)
    ring_c[2].begin_all()
    cross_x_done(1)
    ring_e[0].begin_all()
    own_z_done()
    cross(3)
    ring_c[3].begin_all()
    run(ring_c[2], 0)
    run(ring_e[0], 0)
    run(ring_f, 0)
    cross(4)
    ring_c[4].begin_all()
    run(ring_c[3], 0)
    cross_x_done(2)
    run(ring_e[0], 1)
    run(ring_c[4], 0)
    own_x_done()
    cross_x_done(3)
    cross_x_done(4)
    ring_e[1].begin_all()
    run(ring_e[0], 2)
    run(ring_e[1], 0)
    own_h_done()
    run(ring_e[0], 3)
    run(ring_e[1], 1)
    run(ring_e[0], 4)
    run(ring_e[1], 2)
    cross_z_done(0)
    run(ring_e[1], 3)
    run(ring_e[1], 4)
    cross_z_done(1)

    @pl.when(div(x, 2) == low)
    def _():
        j = 4 * (x - 2 * low) + div(z, 2)
        p = 2 * lax.rem(z, 2) + h

        @pl.when(jnp.logical_not((z == j) & (x == p)))
        def _():
            remote(in_d, in_d, out_d_sem.at[0], in_d_sem.at[0], {"h": 1 - h}).wait_recv()

        for t in range(5):
            out_ref[:, aligned(lax.rem(j + t, 8) * 128, 128)] = in_d[:, t * 128 : (t + 1) * 128]
        for t in range(1, 4):
            source = lax.rem(j + 8 - t, 8)
            for q in range(4):

                @pl.when(jnp.logical_not((z == source) & (x == q)))
                def _():
                    box = in_dt.at[t - 1, q]
                    remote(box, box, out_dt_sem.at[0, 0], in_dt_sem.at[t - 1, q], {"h": 1 - h}).wait_recv()

            out_ref[:, aligned(source * 128, 128)] = (
                in_dt[t - 1, 0] + in_dt[t - 1, 1] + in_dt[t - 1, 2] + in_dt[t - 1, 3]
            )

    @pl.when(div(x, 2) != low)
    def _():
        for s in range(8):
            for g in range(2):

                @pl.when(jnp.logical_not((h == g) & (2 * x + lax.rem(z, 2) == s)))
                def _():
                    box = in_n.at[g, s]
                    remote(box, box, out_n_sem.at[0, 0], in_n_sem.at[g, s], {"h": 1 - h}).wait_recv()

                box = in_t.at[g, s]
                remote(box, box, out_t_sem.at[0, 0], in_t_sem.at[g, s], {"h": 1 - h}).wait_recv()
            out_ref[:, s * 128 : (s + 1) * 128] = (in_n[0, s] + in_n[1, s]) + (in_t[0, s] + in_t[1, s])

    for j in range(len(CHUNKS)):
        y_copy(j).wait_send()
        s_copy(j, mine).wait_send()
    for ring in (ring_d, ring_f, *ring_c, *ring_e):
        ring.drain()
    for k in range(4):
        b_copy(k).wait_send()
    dh_copy().wait_send()
    for t in range(2):
        for q in range(4):
            t_copy(t, q).wait_send()
            _, own_slot, n_out = n_copy(t, q)

            @pl.when(jnp.logical_not(own_slot))
            def _():
                n_out.wait_send()

    stays, straight = straight_copy()

    @pl.when((h == lax.rem(x, 2)) & jnp.logical_not(stays))
    def _():
        straight.wait_send()

    for t in range(1, 4):
        for k in range(2):
            kept, _, turn = turned_copy(t, k)

            @pl.when(jnp.logical_not(kept))
            def _():
                turn.wait_send()


def per_device(pair_matrix, energies, omega):
    pairs, cols = pair_matrix.shape
    width = cols // 4
    dma = pltpu.SemaphoreType.DMA
    loads, chunks = 6, len(CHUNKS)

    def f32(*shape):
        return pltpu.VMEM(shape, jnp.float32)

    def bf16(*shape):
        return pltpu.VMEM(shape, jnp.bfloat16)

    owned = pl.pallas_call(
        kernel,
        out_shape=jax.ShapeDtypeStruct((32, cols), jnp.float32),
        in_specs=[
            pl.BlockSpec(memory_space=pltpu.VMEM),
            pl.BlockSpec(memory_space=pltpu.SMEM),
            pl.BlockSpec(memory_space=pl.ANY),
        ],
        out_specs=pl.BlockSpec(memory_space=pltpu.VMEM),
        scratch_shapes=[
            bf16(pairs, 13 * 128),
            f32(pairs, 128),
            [bf16(pairs // 2, size) for _, size in CHUNKS],
            bf16(pairs // 2, width),
            f32(8, 128, 640),
            f32(2, 2, 4, 64, 640),
            f32(4, cols, width),
            bf16(2, 2, 2, cols // 2, width),
            bf16(2, 2, 2, cols // 2, width),
            f32(8, 128),
            f32(8, 128),
            f32(8, 128),
            f32(3, 8, 128),
            f32(8, width),
            f32(8, width),
            f32(2, 8, 128, 128),
            f32(2, 2, 2, 4, 64, 128),
            f32(4, 32, 640),
            f32(2, 2, 2, 16, 640),
            f32(2, 128, 128),
            f32(2, 128, 128),
            f32(32, 640),
            f32(32, 640),
            f32(32, 640),
            f32(128, 128),
            f32(3, 128, 128),
            f32(32, 640),
            f32(3, 4, 32, 128),
            f32(2, 8, 32, 128),
            f32(2, 8, 32, 128),
            dma((loads,)),
            dma((chunks,)),
            dma((chunks,)),
            dma((chunks,)),
            dma((chunks,)),
            dma((2, 2, 4)),
            dma((2, 2, 4)),
            dma((chunks, 2, 2, 2)),
            dma((chunks, 2, 2, 2)),
            dma((4,)),
            dma((4,)),
            dma((2, 2, 2, 4)),
            dma((2, 2, 2, 4)),
            dma((2, 2, 2)),
            dma((2, 2, 2)),
            dma((2,)),
            dma((2,)),
            dma((1,)),
            dma((3, 4)),
            dma((2, 8)),
            dma((2, 8)),
            dma((1,)),
            dma((3, 2)),
            dma((2, 4)),
            dma((2, 4)),
        ],
        compiler_params=pltpu.CompilerParams(
            collective_id=0, has_side_effects=True, vmem_limit_bytes=60 * 1024 * 1024
        ),
    )(energies.reshape(pairs // 128, 128), omega, pair_matrix)
    return owned[:, None, :]


def solution(mesh):
    finer = Mesh(mesh.devices.reshape(4, 8, 2, 2, 2), ("x", "z", "h", "l", "f"))
    return jax.shard_map(
        per_device,
        mesh=finer,
        in_specs=(P(ROWS, "l"), P(ROWS), P("f")),
        out_specs=P(ROWS, "f", "l"),
        check_vma=False,
    )
```

```python
import jax
import jax.numpy as jnp
from jax import lax
from jax.experimental import pallas as pl
from jax.experimental.pallas import tpu as pltpu
from jax.sharding import Mesh
from jax.sharding import PartitionSpec as P

MESH = pl.DeviceIdType.MESH
ROWS = ("x", "z", "h")
CHUNKS = ((0, 256), (256, 256), (512, 256), (768, 128), (896, 128))


def gram(left, right):
    return -lax.dot_general(
        left, right, (((0,), (0,)), ((), ())), preferred_element_type=jnp.float32
    )


def aligned(value, size, length=None):
    return pl.ds(pl.multiple_of(value, size), length or size)


class Ring:
    def __init__(self, axis, n, block, inbox, send_sem, recv_sem):
        self.axis, self.n, self.block, self.inbox = axis, n, block, inbox
        self.send_sem, self.recv_sem = send_sem, recv_sem
        self.pos = lax.axis_index(axis)

    def first(self, way, side):
        return self.n // 2 if way == side else self.n // 2 - 1

    def toward(self, way, dist):
        return lax.rem(self.pos + (dist if way == 0 else self.n - dist), self.n)

    def copy(self, way, side, dist):
        return pltpu.make_async_remote_copy(
            src_ref=self.block(self.toward(way, dist), side),
            dst_ref=self.inbox(way, side, dist - 1),
            send_sem=self.send_sem.at[way, side, dist - 1],
            recv_sem=self.recv_sem.at[way, side, dist - 1],
            device_id={self.axis: self.toward(way, 1)},
            device_id_type=MESH,
        )

    def begin(self, way, side):
        self.copy(way, side, self.first(way, side)).start()

    def hop(self, way, side, dist):
        self.copy(way, side, dist + 1).wait_recv()
        held = self.block(self.toward(way, dist), side)
        came = self.inbox(way, side, dist)

        @pl.loop(0, held.shape[0] // 16)
        def _(i):
            rows = aligned(i * 16, 16)
            held[rows, :] = held[rows, :] + came[rows, :]

        self.copy(way, side, dist).start()

    def begin_all(self):
        for way, side in ((0, 0), (1, 1), (0, 1), (1, 0)):
            self.begin(way, side)

    def steps(self):
        out = []
        for dist in range(self.n // 2 - 1, 0, -1):
            out.append(((0, 0, dist), (1, 1, dist)))
            if dist > 1:
                out.append(((0, 1, dist - 1), (1, 0, dist - 1)))
        return out

    def arrived(self):
        for way in range(2):
            for side in range(2):
                self.copy(way, side, 1).wait_recv()

    def drain(self):
        for way in range(2):
            for side in range(2):
                for dist in range(self.first(way, side), 0, -1):
                    self.copy(way, side, dist).wait_send()


class CodedRing(Ring):
    def __init__(self, *ring, staged, scale):
        super().__init__(*ring)
        self.staged, (self.enc, self.dec) = staged, scale

    def copy(self, way, side, dist):
        return pltpu.make_async_remote_copy(
            src_ref=self.staged(way, side, dist - 1),
            dst_ref=self.inbox(way, side, dist - 1),
            send_sem=self.send_sem.at[way, side, dist - 1],
            recv_sem=self.recv_sem.at[way, side, dist - 1],
            device_id={self.axis: self.toward(way, 1)},
            device_id_type=MESH,
        )

    def encode(self, value):
        scaled = value * self.enc[:1, : value.shape[1]]
        power = scaled * scaled
        power = power * power
        power = power * power
        return jnp.where(scaled < 0, -power, power).astype(jnp.bfloat16)

    def decode(self, code):
        power = code.astype(jnp.float32)
        fourth = lax.rsqrt(lax.rsqrt(jnp.maximum(jnp.abs(power), 1e-37)))
        root = fourth * lax.rsqrt(fourth) * self.dec[:1, : code.shape[1]]
        return jnp.where(power < 0, -root, root)

    def stage(self, way, side, dist, came=None):
        held = self.block(self.toward(way, dist), side)
        staged = self.staged(way, side, dist - 1)

        @pl.loop(0, held.shape[0] // 64)
        def _(i):
            rows = aligned(i * 64, 64)
            value = held[rows, :]
            if came is not None:
                value = value + self.decode(came[rows, :])
            staged[rows, :] = self.encode(value)

        self.copy(way, side, dist).start()

    def begin(self, way, side):
        self.stage(way, side, self.first(way, side))

    def hop(self, way, side, dist):
        self.copy(way, side, dist + 1).wait_recv()
        self.stage(way, side, dist, self.inbox(way, side, dist))


def kernel(
    e_ref,
    w_ref,
    x_hbm,
    out_ref,
    own,
    fac,
    raw,
    other,
    d_part,
    d_box,
    c_part,
    c_box,
    c_code,
    b_own,
    b_low,
    b_both,
    b_far,
    enc,
    dec,
    e_part,
    e_box,
    f_part,
    f_box,
    tile,
    tile_t,
    d_sum,
    d_sum_box,
    d_fin,
    pad,
    turned,
    in_d,
    in_dt,
    in_n,
    in_t,
    load_sem,
    y_send,
    y_recv,
    s_send,
    s_recv,
    d_send,
    d_recv,
    c_send,
    c_recv,
    b_send,
    b_recv,
    e_send,
    e_recv,
    f_send,
    f_recv,
    h_send,
    h_recv,
    in_d_sem,
    in_dt_sem,
    in_n_sem,
    in_t_sem,
    out_d_sem,
    out_dt_sem,
    out_n_sem,
    out_t_sem,
):
    x, z, h = lax.axis_index("x"), lax.axis_index("z"), lax.axis_index("h")
    low, core = lax.axis_index("l"), lax.axis_index("f")
    pairs, cols = x_hbm.shape
    half, width = pairs // 2, cols // 4
    quarter = half // 2
    wide = d_part.shape[2]
    div = lax.div

    barrier = pltpu.get_barrier_semaphore()
    peers = (
        {"x": lax.rem(x + 1, 4)},
        {"x": lax.rem(x + 2, 4)},
        {"x": lax.rem(x + 3, 4)},
        {"x": lax.rem(x + 3, 4), "l": 1 - low},
        {"z": lax.rem(z + 1, 8)},
        {"z": lax.rem(z + 7, 8)},
        {"h": 1 - h},
        {"l": 1 - low},
        {"f": 1 - core},
    )
    for peer in peers:
        pl.semaphore_signal(barrier, inc=1, device_id=peer, device_id_type=MESH)
    pl.semaphore_wait(barrier, len(peers))

    mine = aligned(core * quarter, quarter)
    theirs = aligned((1 - core) * quarter, quarter)
    leaving = aligned((1 - low) * half + core * quarter, quarter)

    def remote(src, dst, send, recv, peer):
        return pltpu.make_async_remote_copy(
            src_ref=src, dst_ref=dst, send_sem=send, recv_sem=recv, device_id=peer, device_id_type=MESH
        )

    def y_copy(j):
        src = x_hbm.at[leaving, pl.ds(*CHUNKS[j])]
        return remote(src, raw[j].at[mine], y_send.at[j], y_recv.at[j], {"l": 1 - low})

    def s_copy(j, rows):
        return remote(raw[j].at[rows], raw[j].at[rows], s_send.at[j], s_recv.at[j], {"f": 1 - core})

    for j in range(len(CHUNKS)):
        y_copy(j).start()
    loads = load_sem.shape[0]
    block = pairs // loads

    def load(b):
        rows = pl.ds(b * block, block)
        return pltpu.make_async_copy(x_hbm.at[rows], own.at[rows, pl.ds(0, cols)], load_sem.at[b])

    for b in range(loads):
        load(b).start()

    freq = w_ref[0]

    @pl.loop(0, pairs // 128)
    def _(b):
        energy = e_ref[pl.ds(b, 1), :]
        value = jnp.sqrt(4.0 * energy / (energy * energy + freq * freq))
        fac[aligned(b * 128, 128), :] = jnp.broadcast_to(value, (128, 128)).T

    for b in range(loads):
        load(b).wait()

        @pl.loop(0, block // 64)
        def _(i):
            rows = aligned(b * block + i * 64, 64)
            scale = fac[rows, :]
            for c in range(cols // 128):
                lanes = pl.ds(c * 128, 128)
                scaled = (scale * own[rows, lanes].astype(jnp.float32)).astype(jnp.bfloat16)
                own[rows, lanes] = scaled
                if c < 5:
                    own[rows, pl.ds(cols + c * 128, 128)] = scaled

    ring_d = Ring(
        "z", 8, lambda d, s: d_part.at[d, pl.ds(s * 64, 64)], lambda *i: d_box.at[*i], d_send, d_recv
    )
    ring_f = Ring(
        "x", 4, lambda d, s: f_part.at[d, pl.ds(s * 16, 16)], lambda *i: f_box.at[*i], f_send, f_recv
    )

    def ring_of_chunk(j):
        first, size = CHUNKS[j]
        mid = size // 2

        def block(d, s):
            return c_part.at[d, pl.ds(first + s * mid, mid)]

        def inbox(way, side, k):
            return c_box.at[way, side, k, pl.ds(first // 2, mid)]

        def staged(way, side, k):
            return c_code.at[way, side, k, pl.ds(first // 2, mid)]

        return CodedRing(
            "x", 4, block, inbox, c_send.at[j], c_recv.at[j], staged=staged, scale=(enc, dec)
        )

    ring_c = [ring_of_chunk(j) for j in range(len(CHUNKS))]
    ring_e = [
        Ring(
            "z",
            8,
            lambda d, s, t=t: e_part.at[t, d, pl.ds(s * 64, 64)],
            lambda *i, t=t: e_box.at[t, *i],
            e_send.at[t],
            e_recv.at[t],
        )
        for t in range(2)
    ]

    def run(ring, step):
        for way, side, dist in ring.steps()[step]:
            ring.hop(way, side, dist)

    def own_pair(way, dist):
        one = ring_d.toward(way, dist)
        two = lax.rem(one + 1, 8)
        block = gram(own[:, aligned(one * 128, 128, 256)], own[:, aligned(one * 128, 128, wide + 128)])
        d_part[one] = block[:128, :wide]
        d_part[two] = block[128:, 128:]

    mine_half = aligned(low * half, half)

    def cross(j):
        first, size = CHUNKS[j]
        y_copy(j).wait_recv()
        s_copy(j, mine).start()
        s_copy(j, theirs).wait_recv()

        @pl.loop(0, half // 64)
        def _(i):
            rows = aligned(i * 64, 64)
            scale = fac[aligned(low * half + i * 64, 64), :]
            for c in range(size // 128):
                lanes = pl.ds(c * 128, 128)
                other[rows, lanes] = (scale * raw[j][rows, lanes].astype(jnp.float32)).astype(jnp.bfloat16)

        block = gram(other[:, :size], own[mine_half, :cols])
        for d in range(4):
            c_part[d, pl.ds(first, size), :] = block[:, d * width : (d + 1) * width]

    def b_copy(k):
        if k == 0:
            return remote(b_own, b_low, b_send.at[0], b_recv.at[0], {"x": lax.rem(x + 1, 4), "l": 1 - low})
        return remote(b_both, b_far.at[k - 1], b_send.at[k], b_recv.at[k], {"x": lax.rem(x + k, 4)})

    def bound_own():
        most = jnp.abs(d_part[0, :, :128])
        for d in range(1, 8):
            most = jnp.maximum(most, jnp.abs(d_part[d, :, :128]))
        b_own[...] = jnp.full(b_own.shape, jnp.max(most), jnp.float32)
        b_copy(0).start()

    def bound_both():
        b_copy(0).wait_recv()
        b_both[...] = jnp.maximum(b_own[...], b_low[...])
        for k in range(1, 4):
            b_copy(k).start()

    def bound_all():
        most = b_both[...]
        for k in range(1, 4):
            b_copy(k).wait_recv()
            most = jnp.maximum(most, b_far[k - 1])
        most = jnp.broadcast_to(4.0 * jnp.maximum(most[:1, :], 1e-30), (8, 128))
        for c in range(2):
            enc[:, c * 128 : (c + 1) * 128] = 32768.0 / most
            dec[:, c * 128 : (c + 1) * 128] = most / 32768.0

    def cross_x_done(j):
        first, size = CHUNKS[j]
        mid = size // 2
        ring_c[j].arrived()
        for side in range(2):
            start = first + side * mid
            for c in range(2):
                lanes = pl.ds(c * 128, 128)

                @pl.loop(0, mid // 64)
                def _(i):
                    rows = aligned(first // 2 + i * 64, 64)
                    e_part[start // 512, 2 * (start % 512 // 128) + c, aligned(start % 128 + i * 64, 64), :] = (
                        c_part[x, aligned(start + i * 64, 64), lanes]
                        + ring_c[j].decode(c_box[0, side, 0, rows, lanes])
                        + ring_c[j].decode(c_box[1, side, 0, rows, lanes])
                    )

    def n_copy(t, q):
        peer = {"x": 2 * (1 - low) + t, "z": 2 * div(z, 2) + q // 2, "h": jnp.int32(q % 2)}
        slot = 2 * x + lax.rem(z, 2)
        own_slot = (peer["x"] == x) & (peer["z"] == z) & (peer["h"] == h)
        return slot, own_slot, remote(
            tile.at[t, pl.ds(32 * q, 32)], in_n.at[h, slot], out_n_sem.at[t, q], in_n_sem.at[h, slot], peer
        )

    def t_copy(t, q):
        peer = {
            "x": 2 * low + div(x, 2),
            "z": 4 * lax.rem(x, 2) + 2 * lax.rem(z, 2) + q // 2,
            "h": jnp.int32(q % 2),
            "l": 1 - low,
        }
        slot = 4 * t + div(z, 2)
        return remote(
            tile_t.at[t, pl.ds(32 * q, 32)], in_t.at[h, slot], out_t_sem.at[t, q], in_t_sem.at[h, slot], peer
        )

    def cross_z_done(t):
        ring = ring_e[t]
        ring.arrived()
        for side in range(2):

            @pl.loop(0, 4)
            def _(i):
                rows = aligned(i * 16, 16)
                into = aligned(side * 64 + i * 16, 16)
                tile[t, into, :] = (
                    e_part[t, z, into, :] + e_box[t, 0, side, 0, rows, :] + e_box[t, 1, side, 0, rows, :]
                )

        tile_t[t] = tile[t].T
        for q in range(4):
            t_copy(t, q).start()
            slot, own_slot, copy = n_copy(t, q)

            @pl.when(jnp.logical_not(own_slot))
            def _():
                copy.start()

            @pl.when(own_slot)
            def _():
                in_n[h, slot] = tile[t, pl.ds(32 * q, 32), :]

    def own_z_done():
        ring_d.arrived()
        for side in range(2):
            for part in range(2):
                d = 2 * side + part

                @pl.loop(0, 2)
                def _(i):
                    rows = aligned(part * 32 + i * 16, 16)
                    f_part[d, aligned(i * 16, 16), :] = (
                        d_part[z, aligned(d * 32 + i * 16, 16), :]
                        + d_box[0, side, 0, rows, :]
                        + d_box[1, side, 0, rows, :]
                    )

        ring_f.begin_all()

    def dh_copy():
        return remote(d_sum, d_sum_box, h_send.at[1], h_recv.at[1], {"h": 1 - h})

    def own_x_done():
        ring_f.arrived()
        for side in range(2):
            rows = pl.ds(side * 16, 16)
            d_sum[rows, :] = f_part[x, rows, :] + f_box[0, side, 0] + f_box[1, side, 0]
        dh_copy().start()

    def straight_copy():
        peer = {"x": 2 * low + div(z, 4), "z": 2 * lax.rem(z, 4) + div(x, 2)}
        stays = (peer["x"] == x) & (peer["z"] == z)
        return stays, remote(d_fin, in_d, out_d_sem.at[0], in_d_sem.at[0], peer)

    def turned_copy(t, k):
        j = lax.rem(z + t, 8)
        peer = {"x": 2 * low + div(j, 4), "z": 2 * lax.rem(j, 4) + k}
        stays = (peer["x"] == x) & (peer["z"] == z)
        src = turned.at[t - 1, aligned(64 * k + 32 * h, 32)]
        return stays, src, remote(src, in_dt.at[t - 1, x], out_dt_sem.at[t - 1, k], in_dt_sem.at[t - 1, x], peer)

    def own_h_done():
        dh_copy().wait_recv()
        d_fin[...] = d_sum[...] + d_sum_box[...]

        @pl.when(h == lax.rem(x, 2))
        def _():
            stays, copy = straight_copy()

            @pl.when(jnp.logical_not(stays))
            def _():
                copy.start()

            @pl.when(stays)
            def _():
                in_d[...] = d_fin[...]

        pad[...] = jnp.zeros_like(pad)
        for t in range(1, 4):
            pad[aligned(x * 32, 32), :] = d_fin[:, t * 128 : (t + 1) * 128]
            turned[t - 1] = pad[...].T
            for k in range(2):
                stays, src, copy = turned_copy(t, k)

                @pl.when(jnp.logical_not(stays))
                def _():
                    copy.start()

                @pl.when(stays)
                def _():
                    in_dt[t - 1, x] = src[...]

    own_pair(0, 3)
    ring_d.begin(0, 0)
    ring_d.begin(1, 1)
    ring_d.begin(0, 1)
    own_pair(1, 3)
    ring_d.begin(1, 0)
    own_pair(0, 1)
    own_pair(1, 1)
    bound_own()
    cross(0)
    bound_both()
    run(ring_d, 0)
    bound_all()
    ring_c[0].begin_all()
    run(ring_d, 1)
    run(ring_c[0], 0)
    cross(1)
    ring_c[1].begin_all()
    run(ring_d, 2)
    cross_x_done(0)
    run(ring_d, 3)
    run(ring_c[1], 0)
    run(ring_d, 4)
    cross(2)
    ring_c[2].begin_all()
    cross_x_done(1)
    ring_e[0].begin_all()
    own_z_done()
    cross(3)
    ring_c[3].begin_all()
    run(ring_c[2], 0)
    run(ring_e[0], 0)
    run(ring_f, 0)
    cross(4)
    ring_c[4].begin_all()
    run(ring_c[3], 0)
    cross_x_done(2)
    run(ring_e[0], 1)
    run(ring_c[4], 0)
    own_x_done()
    cross_x_done(3)
    cross_x_done(4)
    ring_e[1].begin_all()
    run(ring_e[0], 2)
    run(ring_e[1], 0)
    run(ring_e[0], 3)
    run(ring_e[1], 1)
    run(ring_e[0], 4)
    run(ring_e[1], 2)
    run(ring_e[1], 3)
    own_h_done()
    cross_z_done(0)
    run(ring_e[1], 4)
    cross_z_done(1)

    @pl.when(div(x, 2) == low)
    def _():
        j = 4 * (x - 2 * low) + div(z, 2)
        p = 2 * lax.rem(z, 2) + h

        @pl.when(jnp.logical_not((z == j) & (x == p)))
        def _():
            remote(in_d, in_d, out_d_sem.at[0], in_d_sem.at[0], {"h": 1 - h}).wait_recv()

        for t in range(5):
            out_ref[:, aligned(lax.rem(j + t, 8) * 128, 128)] = in_d[:, t * 128 : (t + 1) * 128]
        for t in range(1, 4):
            source = lax.rem(j + 8 - t, 8)
            for q in range(4):

                @pl.when(jnp.logical_not((z == source) & (x == q)))
                def _():
                    box = in_dt.at[t - 1, q]
                    remote(box, box, out_dt_sem.at[0, 0], in_dt_sem.at[t - 1, q], {"h": 1 - h}).wait_recv()

            out_ref[:, aligned(source * 128, 128)] = (
                in_dt[t - 1, 0] + in_dt[t - 1, 1] + in_dt[t - 1, 2] + in_dt[t - 1, 3]
            )

    @pl.when(div(x, 2) != low)
    def _():
        for s in range(8):
            for g in range(2):

                @pl.when(jnp.logical_not((h == g) & (2 * x + lax.rem(z, 2) == s)))
                def _():
                    box = in_n.at[g, s]
                    remote(box, box, out_n_sem.at[0, 0], in_n_sem.at[g, s], {"h": 1 - h}).wait_recv()

                box = in_t.at[g, s]
                remote(box, box, out_t_sem.at[0, 0], in_t_sem.at[g, s], {"h": 1 - h}).wait_recv()
            out_ref[:, s * 128 : (s + 1) * 128] = (in_n[0, s] + in_n[1, s]) + (in_t[0, s] + in_t[1, s])

    for j in range(len(CHUNKS)):
        y_copy(j).wait_send()
        s_copy(j, mine).wait_send()
    for ring in (ring_d, ring_f, *ring_c, *ring_e):
        ring.drain()
    for k in range(4):
        b_copy(k).wait_send()
    dh_copy().wait_send()
    for t in range(2):
        for q in range(4):
            t_copy(t, q).wait_send()
            _, own_slot, n_out = n_copy(t, q)

            @pl.when(jnp.logical_not(own_slot))
            def _():
                n_out.wait_send()

    stays, straight = straight_copy()

    @pl.when((h == lax.rem(x, 2)) & jnp.logical_not(stays))
    def _():
        straight.wait_send()

    for t in range(1, 4):
        for k in range(2):
            kept, _, turn = turned_copy(t, k)

            @pl.when(jnp.logical_not(kept))
            def _():
                turn.wait_send()


def per_device(pair_matrix, energies, omega):
    pairs, cols = pair_matrix.shape
    width = cols // 4
    dma = pltpu.SemaphoreType.DMA
    loads, chunks = 6, len(CHUNKS)

    def f32(*shape):
        return pltpu.VMEM(shape, jnp.float32)

    def bf16(*shape):
        return pltpu.VMEM(shape, jnp.bfloat16)

    owned = pl.pallas_call(
        kernel,
        out_shape=jax.ShapeDtypeStruct((32, cols), jnp.float32),
        in_specs=[
            pl.BlockSpec(memory_space=pltpu.VMEM),
            pl.BlockSpec(memory_space=pltpu.SMEM),
            pl.BlockSpec(memory_space=pl.ANY),
        ],
        out_specs=pl.BlockSpec(memory_space=pltpu.VMEM),
        scratch_shapes=[
            bf16(pairs, 13 * 128),
            f32(pairs, 128),
            [bf16(pairs // 2, size) for _, size in CHUNKS],
            bf16(pairs // 2, width),
            f32(8, 128, 640),
            f32(2, 2, 4, 64, 640),
            f32(4, cols, width),
            bf16(2, 2, 2, cols // 2, width),
            bf16(2, 2, 2, cols // 2, width),
            f32(8, 128),
            f32(8, 128),
            f32(8, 128),
            f32(3, 8, 128),
            f32(8, width),
            f32(8, width),
            f32(2, 8, 128, 128),
            f32(2, 2, 2, 4, 64, 128),
            f32(4, 32, 640),
            f32(2, 2, 2, 16, 640),
            f32(2, 128, 128),
            f32(2, 128, 128),
            f32(32, 640),
            f32(32, 640),
            f32(32, 640),
            f32(128, 128),
            f32(3, 128, 128),
            f32(32, 640),
            f32(3, 4, 32, 128),
            f32(2, 8, 32, 128),
            f32(2, 8, 32, 128),
            dma((loads,)),
            dma((chunks,)),
            dma((chunks,)),
            dma((chunks,)),
            dma((chunks,)),
            dma((2, 2, 4)),
            dma((2, 2, 4)),
            dma((chunks, 2, 2, 2)),
            dma((chunks, 2, 2, 2)),
            dma((4,)),
            dma((4,)),
            dma((2, 2, 2, 4)),
            dma((2, 2, 2, 4)),
            dma((2, 2, 2)),
            dma((2, 2, 2)),
            dma((2,)),
            dma((2,)),
            dma((1,)),
            dma((3, 4)),
            dma((2, 8)),
            dma((2, 8)),
            dma((1,)),
            dma((3, 2)),
            dma((2, 4)),
            dma((2, 4)),
        ],
        compiler_params=pltpu.CompilerParams(
            collective_id=0, has_side_effects=True, vmem_limit_bytes=60 * 1024 * 1024
        ),
    )(energies.reshape(pairs // 128, 128), omega, pair_matrix)
    return owned[:, None, :]


def solution(mesh):
    finer = Mesh(mesh.devices.reshape(4, 8, 2, 2, 2), ("x", "z", "h", "l", "f"))
    return jax.shard_map(
        per_device,
        mesh=finer,
        in_specs=(P(ROWS, "l"), P(ROWS), P("f")),
        out_specs=P(ROWS, "f", "l"),
        check_vma=False,
    )
```
